128 devices in a mesh: scen: 32 (over z, y_lo, x), fac: 4 (over y_hi, core).
Axes of the slice: x: 4, y: 4 (y_hi: 2, y_lo: 2; y = y_hi * 2 + y_lo), z: 4, core: 2. Of those that a mesh axis runs over, the one named last changes fastest.
Arguments:
- scenario_draws: bfloat16 [32768, 4096], P('scen'), may hold values from -6 to 6
- cholesky: bfloat16 [4096, 4096], P('scen', 'fac'), may hold values from -1.5 to 1.5, as said below
- exposures: bfloat16 [4096, 4096], P('fac'), may hold values from -0.09375 to 0.09375
- drift: float32 [4096], P('fac'), may hold values from -3 to 3
Outputs:
- covariance: float32 [4096, 4096], P('scen', 'fac')
- expected: float32 [4096], P('fac')
The draws below stay inside these ranges and needn't reach their ends.
Inputs may be any that keep to these rules, and one draw needn't show every extreme that they name: cholesky is lower triangular (zero above the diagonal) with diagonal entries of 0.5 to 1.5.
All inputs are finite; a program needn't handle non-finite values.
Results may differ from the reference program's by a relative error of at most 0.0013.
Values may be sent and summed in bfloat16 or wider, within the bound.
No kernel may reach another device: no remote copies, remote signals or barrier semaphores. Data moves between devices by JAX's collectives and lax.ppermute only.
A program may use at most 128 MiB of HBM per device.

```python
import jax
import jax.numpy as jnp
from jax import lax

F = 4096
DESKS = 4096
SCEN = 32768


def draw_cholesky(key, part):
    key_low, key_diag = jax.random.split(jax.random.fold_in(key, 7))
    below = jax.random.truncated_normal(key_low, -4.0, 4.0, (F, F), jnp.float32) / jnp.sqrt(jnp.float32(F))
    lower = jnp.tril(below, -1)
    diag_vals = jax.random.uniform(key_diag, (F,), jnp.float32, 0.5, 1.5)
    return (lower + jnp.diag(diag_vals)).astype(jnp.bfloat16)


def shard_levels(key, shape, cuts, smallest, high):
    loudness = 1.0
    for axis_at, blocks in cuts:
        draws = jax.random.uniform(jax.random.fold_in(jax.random.fold_in(key, 6), axis_at), (blocks,), jnp.float32, smallest / len(cuts), high / len(cuts))
        loudness = loudness * jnp.repeat(jnp.exp(draws), shape[axis_at] // blocks).reshape((-1,) + (1,) * (len(shape) - 1 - axis_at))
    return loudness


def normal_values(rng, shape, spread, reach, cuts=(), held_as=jnp.bfloat16):
    gain = shard_levels(rng, shape, cuts, -0.22, 0.18) if cuts else 1.0
    result = jax.random.normal(rng, shape, jnp.float32) * spread * gain
    return jnp.minimum(jnp.maximum(result, -reach), reach).astype(held_as)


def setup_inputs(seed: int = 0) -> dict:
    arg_keys = jax.random.split(jax.random.key(seed), 5)
    return {
        "scenario_draws": normal_values(arg_keys[0], (SCEN, F), 1.0, 6.0, ((0, 32),)),
        "cholesky": draw_cholesky(jax.random.fold_in(arg_keys[4], 71), 0),
        "exposures": normal_values(arg_keys[2], (DESKS, F), F ** -0.5, 0.09375, ((0, 4),)),
        "drift": normal_values(arg_keys[3], (F,), 0.5, 3.0, ((0, 4),), jnp.float32),
    }


def reference(scenario_draws, cholesky, exposures, drift):
    mixed = jnp.dot(scenario_draws, cholesky, preferred_element_type=jnp.float32)
    shocks = (mixed + drift[None, :]).astype(jnp.bfloat16)
    pnl = lax.dot_general(shocks, exposures, (((1,), (1,)), ((), ())), preferred_element_type=jnp.float32).astype(jnp.bfloat16)
    expected = jnp.sum(pnl, axis=0, dtype=jnp.float32) / SCEN
    gram = lax.dot_general(pnl, pnl, (((0,), (0,)), ((), ())), preferred_element_type=jnp.float32)
    covariance = (gram - SCEN * expected[:, None] * expected[None, :]) / (SCEN - 1)
    return covariance, expected
```

```python
import jax
import jax.numpy as jnp
from jax import lax
from jax.sharding import Mesh
from jax.sharding import PartitionSpec as P

SCEN = ("z", "yl", "x")
FAC = ("yh", "c")
F32, F16, BF16 = jnp.float32, jnp.float16, jnp.bfloat16
G_SCALE = 1.0 / 32.0
V_SCALE = 64.0


def dot(a, b, ca, cb):
    return lax.dot_general(a, b, (((ca,), (cb,)), ((), ())), preferred_element_type=F32)


def split(x):
    hi = lax.reduce_precision(x, 8, 7)
    return hi.astype(BF16), (x - hi).astype(BF16)


def dot3(a, b, ca, cb):
    (ah, al), (bh, bl) = a, b
    return dot(ah, bh, ca, cb) + (dot(ah, bl, ca, cb) + dot(al, bh, ca, cb))


def shift(x, axis, k):
    n = lax.axis_size(axis)
    return lax.ppermute(x, axis, [(i, (i + k) % n) for i in range(n)])


def flip(x, axis):
    return lax.ppermute(x, axis, [(0, 1), (1, 0)])


def add(*xs):
    total = xs[0].astype(F32)
    for v in xs[1:]:
        total = total + v.astype(F32)
    return total


def ring_reduce(far, right, left, own, axis):
    half = far.shape[0] // 2
    via_right = shift(far[:half], axis, 1)
    via_left = shift(far[half:], axis, -1)
    to_right = jnp.concatenate([add(right[:half], via_right).astype(F16), right[half:]])
    to_left = jnp.concatenate([left[:half], add(left[half:], via_left).astype(F16)])
    from_left = shift(to_right, axis, 1)
    from_right = shift(to_left, axis, -1)
    return add(own, from_left, from_right)


def ring_gather(x, axis):
    i = lax.axis_index(axis)
    half = x.shape[0] // 2
    prev = shift(x, axis, 1)
    nxt = shift(x, axis, -1)
    far = jnp.concatenate([shift(prev[:half], axis, 1), shift(nxt[half:], axis, -1)])
    out = jnp.zeros((4, *x.shape), x.dtype)
    for k, v in ((0, x), (3, prev), (1, nxt), (2, far)):
        out = lax.dynamic_update_slice_in_dim(out, v[None], (i + k) % 4, 0)
    return out


def pair_gather(x, axis):
    i = lax.axis_index(axis)
    other = flip(x, axis)
    first = jnp.where(i == 0, x, other)
    second = jnp.where(i == 0, other, x)
    return jnp.stack([first, second])


def total_over(x, axes):
    for axis in axes:
        x = x + flip(x, axis) if lax.axis_size(axis) == 2 else four_sum(x, axis)
    return x


def four_sum(x, axis):
    x = x + lax.ppermute(x, axis, [(0, 1), (1, 0), (2, 3), (3, 2)])
    return x + lax.ppermute(x, axis, [(0, 3), (3, 0), (1, 2), (2, 1)])


def pack(x):
    top = jnp.max(jnp.abs(x))
    e = jnp.clip(jnp.floor(jnp.log2(jnp.maximum(top, 1e-30))), -100.0, 120.0)
    body = (x * jnp.exp2(13.0 - e)).astype(F16)
    tail = jnp.broadcast_to(e.astype(F16), (*x.shape[:-2], 16, x.shape[-1]))
    return jnp.concatenate([body, tail], axis=-2)


def unpack(y):
    e = y[..., -16:-15, :].astype(F32)
    return y[..., :-16, :].astype(F32) * jnp.exp2(e - 13.0)


def on_device(draws, chol, exposures, drift):
    z, yl, x = (lax.axis_index(k) for k in SCEN)
    f = lax.axis_index(FAC)
    rows = draws.shape[0]
    total = rows * 32
    draw_sums = total_over(jnp.sum(draws, axis=0, dtype=F32), ("x", "z", "yl"))

    quarter = chol.shape[1]
    chol_rows = lax.all_gather(chol, FAC, axis=1, tiled=True)
    v_own = dot(exposures, chol_rows, 1, 1)
    v16 = (v_own * V_SCALE).astype(F16)

    s = lax.axis_index(SCEN)
    means = draw_sums / total
    drift_all = lax.all_gather(drift, FAC, axis=0, tiled=True)
    part = jnp.sum(v_own * lax.dynamic_slice_in_dim(means, s * 128, 128)[None, :], axis=1) + jnp.sum(
        lax.dynamic_slice_in_dim(exposures, s * 128, 128, 1).astype(F32)
        * lax.dynamic_slice_in_dim(drift_all, s * 128, 128)[None, :],
        axis=1,
    )
    expected = total_over(part, ("x", "z", "yl"))

    tiles = draws.reshape(rows, 4, 2, 4, 128)
    columns = lax.dynamic_slice_in_dim(draws, f * quarter, quarter, 1)
    col_tiles = columns.reshape(rows, 2, 4, 128)
    k_a = tiles[:, :, :, :2].reshape(rows, 2048)
    k_b = tiles[:, :, :, 2:]

    def chunk_a(q):
        part_cols = lax.dynamic_slice_in_dim(col_tiles, q % 4, 1, 2).reshape(rows, 256)
        return (dot(k_a, part_cols, 0, 0) * G_SCALE).astype(F16)

    def chunk_b(q):
        part_rows = lax.dynamic_slice_in_dim(k_b, q % 4, 1, 1).reshape(rows, 512)
        return (dot(part_rows, columns, 0, 0) * G_SCALE).astype(F16)

    a1 = ring_reduce(chunk_a(x + 2), chunk_a(x + 1), chunk_a(x + 3), chunk_a(x), "x")
    b1 = ring_reduce(chunk_b(z + 2), chunk_b(z + 1), chunk_b(z + 3), chunk_b(z), "z")
    a1 = a1.astype(F16).reshape(4, 512, 256)
    b1 = b1.astype(F16).reshape(512, 2, 4, 128)

    def part_a(q):
        return lax.dynamic_index_in_dim(a1, q % 4, 0, False)

    def part_b(q):
        return lax.dynamic_index_in_dim(b1, q % 4, 2, False).reshape(512, 256)

    a2 = ring_reduce(part_a(z + 2), part_a(z + 1), part_a(z + 3), part_a(z), "z")
    b2 = ring_reduce(part_b(x + 2), part_b(x + 1), part_b(x + 3), part_b(x), "x")
    both = jnp.stack([a2.reshape(2, 256, 256), b2.reshape(2, 256, 256)], axis=1).astype(F16)
    mine = lax.dynamic_index_in_dim(both, yl, 0, False)
    theirs = lax.dynamic_index_in_dim(both, 1 - yl, 0, False)
    gram = add(mine, flip(theirs, "yl")).reshape(512, 256).astype(F16)
    gram = pair_gather(pair_gather(gram, "yh"), "c")
    gram = gram.transpose(2, 1, 0, 3).reshape(512, 1024).astype(F32)
    sums = draw_sums.reshape(4, 2, 4, 128)
    k_sums = lax.dynamic_slice_in_dim(draw_sums, (z * 2 + yl) * 512, 512)
    l_sums = lax.dynamic_index_in_dim(sums, x, 2, False).reshape(1024)
    cov_z = (gram / G_SCALE - k_sums[:, None] * (l_sums / total)[None, :]) / (total - 1)

    v1 = ring_gather(pair_gather(v16, "yl"), "z")
    v1 = v1.transpose(2, 0, 1, 3).reshape(1024, 1024).astype(F32) / V_SCALE
    v1 = split(v1)

    t_part = dot3(split(cov_z), v1, 1, 1)
    t = unpack(lax.all_to_all(pack(t_part.reshape(4, 128, 1024)), "x", 0, 0, tiled=True)).sum(axis=0)
    t16 = pack(t.reshape(128, 2, 512).transpose(1, 0, 2))
    got = jnp.zeros((4, 2, *t16.shape[1:]), F16)
    group = ("z", "yl", "yh", "c")
    for d in range(2):
        block = lax.dynamic_index_in_dim(t16, yl ^ d, 0, False)
        for j in range(4):
            pairs = []
            for zz in range(4):
                for yy in range(2):
                    for ff in range(4):
                        pairs.append((zz * 8 + yy * 4 + ff, ff * 8 + (yy ^ d) * 4 + (zz + j) % 4))
            r = lax.ppermute(block, group, pairs)
            got = lax.dynamic_update_slice(got, r[None, None], ((f - j) % 4, yl ^ d, 0, 0))
    t_rows = split(unpack(got).reshape(1024, 512))
    cov_part = dot3(t_rows, v1, 0, 1)
    cov = unpack(lax.all_to_all(pack(cov_part.reshape(4, 128, 1024)), "x", 0, 0, tiled=True)).sum(axis=0)
    return cov, expected


def solution(mesh):
    torus = Mesh(mesh.devices.reshape(4, 2, 4, 2, 2), ("z", "yl", "x", "yh", "c"))
    in_specs = (P(SCEN, None), P(SCEN, FAC), P(FAC, None), P(FAC))
    out_specs = (P(SCEN, FAC), P(FAC))
    return jax.shard_map(
        on_device, mesh=torus, in_specs=in_specs, out_specs=out_specs, check_vma=False
    )
```

```python
import jax
import jax.numpy as jnp
from jax import lax
from jax.sharding import Mesh
from jax.sharding import PartitionSpec as P

SCEN = ("z", "yl", "x")
FAC = ("yh", "c")
F32, F16, BF16 = jnp.float32, jnp.float16, jnp.bfloat16
G_SCALE = 1.0 / 32.0
V_SCALE = 64.0
fence = lax.optimization_barrier


def dot(a, b, ca, cb):
    return lax.dot_general(a, b, (((ca,), (cb,)), ((), ())), preferred_element_type=F32)


def split(x):
    hi = lax.reduce_precision(x, 8, 7)
    return hi.astype(BF16), (x - hi).astype(BF16)


def shift(x, axis, k):
    n = lax.axis_size(axis)
    return lax.ppermute(x, axis, [(i, (i + k) % n) for i in range(n)])


def flip(x, axis):
    return lax.ppermute(x, axis, [(0, 1), (1, 0)])


def add(*xs):
    total = xs[0].astype(F32)
    for v in xs[1:]:
        total = total + v.astype(F32)
    return total


def cols(x, start, size):
    return lax.dynamic_slice_in_dim(x, start, size, 1)


def ring_reduce(part, axis):
    a_far = shift(part(0, 2), axis, 1)
    b_far = shift(part(1, 2), axis, -1)
    a_left = shift(part(0, 3), axis, -1)
    b_right = shift(part(1, 1), axis, 1)
    a_right = shift(add(part(0, 1), a_far).astype(F16), axis, 1)
    b_left = shift(add(part(1, 3), b_far).astype(F16), axis, -1)
    return (
        add(part(0, 0), a_left, a_right).astype(F16),
        add(part(1, 0), b_left, b_right).astype(F16),
    )


def pair(x, axis):
    i = lax.axis_index(axis)
    other = flip(x, axis)
    return jnp.where(i == 0, x, other), jnp.where(i == 0, other, x)


def pack(x, extra=None):
    top = jnp.max(jnp.abs(x))
    if extra is not None:
        top = jnp.maximum(top, jnp.max(jnp.abs(extra)))
    e = jnp.clip(jnp.floor(jnp.log2(jnp.maximum(top, 1e-30))), -100.0, 120.0)
    scale = jnp.exp2(13.0 - e)
    rows = x.shape[-2]
    pads = [(0, 0, 0)] * (x.ndim - 2) + [(0, 16, 0), (0, 0, 0)]
    y = lax.pad(x * scale, jnp.float32(0), pads)
    at = lax.broadcasted_iota(jnp.int32, y.shape, y.ndim - 2)
    y = jnp.where(at == rows, e, y)
    if extra is not None:
        hi = lax.reduce_precision(extra * scale, 5, 10)
        y = jnp.where(at == rows + 1, hi, y)
        y = jnp.where(at == rows + 2, extra * scale - hi, y)
    return y.astype(F16)


def unpack(y):
    rows = y.shape[-2] - 16
    back = jnp.exp2(y[..., rows : rows + 1, :].astype(F32) - 13.0)
    return y[..., :rows, :].astype(F32) * back, (
        y[..., rows + 1 : rows + 2, :].astype(F32) + y[..., rows + 2 : rows + 3, :].astype(F32)
    ) * back


def on_device(draws, chol, exposures, drift):
    z, yl, x = (lax.axis_index(k) for k in SCEN)
    f = lax.axis_index(FAC)
    rows = draws.shape[0]
    total = rows * 32

    d_hi = lax.reduce_precision(drift, 8, 7)
    d_mid = lax.reduce_precision(drift - d_hi, 8, 7)
    d_lo = drift - d_hi - d_mid
    at = lax.broadcasted_iota(jnp.int32, (16, 1024), 0)
    tail = jnp.where(at == 0, d_hi, jnp.where(at == 1, d_mid, jnp.where(at == 2, d_lo, 0.0)))
    own = jnp.concatenate([chol, tail.astype(BF16)], axis=0)
    pieces = [pair(v, "c") for v in pair(own, "yh")]
    lower = jnp.concatenate([v for p in pieces for v in p], axis=1)
    v_own = dot(lower, exposures, 1, 1)
    drift_part = v_own[128] + v_own[129] + v_own[130]
    v16 = (v_own[:128] * V_SCALE).astype(F16)

    v0, v1 = pair(v16, "yl")
    v_pair = jnp.stack([v0, v1])
    v_prev, v_next = shift(v_pair, "z", 1), shift(v_pair, "z", -1)
    v_far = shift(v_prev[0], "z", 1), shift(v_next[1], "z", -1)
    v_all = jnp.zeros((4, *v_pair.shape), F16)
    for k, v in ((0, v_pair), (3, v_prev), (1, v_next), (2, jnp.stack(v_far))):
        v_all = lax.dynamic_update_slice_in_dim(v_all, v[None], (z + k) % 4, 0)
    v_hi, v_lo = split(v_all.reshape(1024, 1024).astype(F32) / V_SCALE)
    v_cat = jnp.concatenate([v_hi, v_lo, v_hi], axis=0)

    wide = cols(draws, f * 1024, 1024)
    ones = jnp.ones((rows, 16), BF16)
    left = [
        jnp.concatenate([draws[:, a * 1024 + h * 256 :][:, :256] for a in range(4)], axis=1)
        for h in range(2)
    ]
    narrow = {}
    for k in range(4):
        q = (x + k) % 4
        narrow[k] = jnp.concatenate([cols(wide, q * 128, 128), cols(wide, 512 + q * 128, 128)], axis=1)

    def gram(a, b):
        return fence((dot(a, b, 0, 0) * G_SCALE).astype(F16))

    part_a, part_b = {}, {}
    for k in (2, 1, 3, 0):
        q = (z + k) % 4
        for h in range(2):
            part_a[h, k] = gram(left[h], narrow[k])
            lhs = cols(draws, q * 1024 + 512 + h * 256, 256)
            part_b[h, k] = gram(jnp.concatenate([lhs, ones], axis=1) if h else lhs, wide)
    a = ring_reduce(lambda h, k: part_a[h, k], "x")
    b = ring_reduce(lambda h, k: part_b[h, k], "z")
    a = ring_reduce(lambda h, k: lax.dynamic_slice_in_dim(a[h], (z + k) % 4 * 256, 256, 0), "z")

    def narrow_b(h, k):
        q = (x + k) % 4
        return jnp.concatenate([cols(b[h], q * 128, 128), cols(b[h], 512 + q * 128, 128)], axis=1)

    b = ring_reduce(narrow_b, "x")
    sums = b[1][256:]
    tile_a = jnp.concatenate([a[0], a[1], sums], axis=0)
    tile_b = jnp.concatenate([b[0], b[1]], axis=0)
    mine = jnp.where(yl == 0, tile_a, tile_b)
    theirs = flip(jnp.where(yl == 0, tile_b, tile_a), "yl")
    tile = add(mine, theirs).astype(F16)
    pieces = [pair(v, "c") for v in pair(tile, "yh")]
    tile = jnp.concatenate([v for p in pieces for v in p], axis=1).astype(F32)
    c_hi, c_lo = split(tile)
    c_cat = jnp.concatenate([c_hi, c_hi, c_lo], axis=1)

    t_part = dot(c_cat, v_cat, 1, 0)
    sent = pack(t_part[:512].reshape(4, 128, 1024), t_part[512:513][None])
    t, mean = unpack(lax.all_to_all(sent, "x", 0, 0, tiled=True))
    t, mean = t.sum(axis=0), mean.sum(axis=0) / (G_SCALE * total)
    own_sums = lax.dynamic_slice(tile, (512, (z * 2 + yl) * 128), (1, 128)).reshape(128, 1)
    t = (t - own_sums * mean) * (1.0 / (G_SCALE * (total - 1)))
    expected = mean[0] + drift_part

    t16 = pack(t)
    got = jnp.zeros((8, 144, 512), F16)
    group = ("z", "yl", "yh", "c")
    for d in range(2):
        block = cols(t16, (yl ^ d) * 512, 512)
        for j in range(4):
            pairs = []
            for zz in range(4):
                for yy in range(2):
                    for ff in range(4):
                        pairs.append((zz * 8 + yy * 4 + ff, ff * 8 + (yy ^ d) * 4 + (zz + j) % 4))
            r = lax.ppermute(block, group, pairs)
            got = lax.dynamic_update_slice_in_dim(got, r[None], ((f - j) % 4) * 2 + (yl ^ d), 0)
    t_hi, t_lo = split(unpack(got)[0].reshape(1024, 512))
    t_cat = jnp.concatenate([t_hi, t_hi, t_lo], axis=0)
    cov_part = dot(t_cat, v_cat, 0, 0)
    cov = unpack(lax.all_to_all(pack(cov_part.reshape(4, 128, 1024)), "x", 0, 0, tiled=True))[0]
    return cov.sum(axis=0), expected


def solution(mesh):
    torus = Mesh(mesh.devices.reshape(4, 2, 4, 2, 2), ("z", "yl", "x", "yh", "c"))
    in_specs = (P(SCEN, None), P(SCEN, FAC), P(FAC, None), P(FAC))
    out_specs = (P(SCEN, FAC), P(FAC))
    return jax.shard_map(
        on_device, mesh=torus, in_specs=in_specs, out_specs=out_specs, check_vma=False
    )
```

```python
import jax
import jax.numpy as jnp
from jax import lax
from jax.sharding import Mesh
from jax.sharding import PartitionSpec as P

SCEN = ("z", "yl", "x")
FAC = ("yh", "c")
F32, F16, BF16 = jnp.float32, jnp.float16, jnp.bfloat16
G_SCALE = 1.0 / 32.0
V_SCALE = 64.0
fence = lax.optimization_barrier


def dot(a, b, ca, cb):
    return lax.dot_general(a, b, (((ca,), (cb,)), ((), ())), preferred_element_type=F32)


def split(x):
    hi = lax.reduce_precision(x, 8, 7)
    return hi.astype(BF16), (x - hi).astype(BF16)


def shift(x, axis, k):
    n = lax.axis_size(axis)
    return lax.ppermute(x, axis, [(i, (i + k) % n) for i in range(n)])


def flip(x, axis):
    return lax.ppermute(x, axis, [(0, 1), (1, 0)])


def add(*xs):
    total = xs[0].astype(F32)
    for v in xs[1:]:
        total = total + v.astype(F32)
    return total


def cols(x, start, size):
    return lax.dynamic_slice_in_dim(x, start, size, 1)


def ring_reduce(plus, minus, both, own, axis, dim):
    cut = both.shape[dim] // 32 * 16
    from_prev = shift(plus, axis, 1)
    from_next = shift(minus, axis, -1)

    def halves(v):
        return lax.slice_in_dim(v, 0, cut, axis=dim), lax.slice_in_dim(v, cut, v.shape[dim], axis=dim)

    b0, b1 = halves(both)
    far0, near1 = halves(from_prev)
    near0, far1 = halves(from_next)
    sum0 = shift(add(b0, far0).astype(F16), axis, 1)
    sum1 = shift(add(b1, far1).astype(F16), axis, -1)
    o0, o1 = halves(own)
    return add(o0, near0, sum0).astype(F16), add(o1, near1, sum1).astype(F16)


def pair(x, axis):
    i = lax.axis_index(axis)
    other = flip(x, axis)
    return jnp.where(i == 0, x, other), jnp.where(i == 0, other, x)


def pack(x, extra=None):
    top = jnp.max(jnp.abs(x))
    if extra is not None:
        top = jnp.maximum(top, jnp.max(jnp.abs(extra)))
    e = jnp.clip(jnp.floor(jnp.log2(jnp.maximum(top, 1e-30))), -100.0, 120.0)
    scale = jnp.exp2(13.0 - e)
    rows = x.shape[-2]
    pads = [(0, 0, 0)] * (x.ndim - 2) + [(0, 16, 0), (0, 0, 0)]
    y = lax.pad(x * scale, jnp.float32(0), pads)
    at = lax.broadcasted_iota(jnp.int32, y.shape, y.ndim - 2)
    y = jnp.where(at == rows, e, y)
    if extra is not None:
        hi = lax.reduce_precision(extra * scale, 5, 10)
        y = jnp.where(at == rows + 1, hi, y)
        y = jnp.where(at == rows + 2, extra * scale - hi, y)
    return y.astype(F16)


def unpack(y):
    rows = y.shape[-2] - 16
    back = jnp.exp2(y[..., rows : rows + 1, :].astype(F32) - 13.0)
    return y[..., :rows, :].astype(F32) * back, (
        y[..., rows + 1 : rows + 2, :].astype(F32) + y[..., rows + 2 : rows + 3, :].astype(F32)
    ) * back


def on_device(draws, chol, exposures, drift):
    z, yl, x = (lax.axis_index(k) for k in SCEN)
    f = lax.axis_index(FAC)
    rows = draws.shape[0]
    total = rows * 32

    d_hi = lax.reduce_precision(drift, 8, 7)
    d_mid = lax.reduce_precision(drift - d_hi, 8, 7)
    d_lo = drift - d_hi - d_mid
    at = lax.broadcasted_iota(jnp.int32, (16, 1024), 0)
    tail = jnp.where(at == 0, d_hi, jnp.where(at == 1, d_mid, jnp.where(at == 2, d_lo, 0.0)))
    own = jnp.concatenate([chol, tail.astype(BF16)], axis=0)
    pieces = [pair(v, "c") for v in pair(own, "yh")]
    lower = jnp.concatenate([v for p in pieces for v in p], axis=1)
    v_own = dot(lower, exposures, 1, 1)
    drift_part = v_own[128] + v_own[129] + v_own[130]
    v16 = (v_own[:128] * V_SCALE).astype(F16)

    v_pair = jnp.concatenate(pair(v16, "yl"), axis=0)
    v_all = jnp.zeros((1024, 1024), F16)
    for k, v in ((0, v_pair), (3, shift(v_pair, "z", 1)), (1, shift(v_pair, "z", -1)), (2, shift(v_pair, "z", 2))):
        v_all = lax.dynamic_update_slice_in_dim(v_all, v, (z + k) % 4 * 256, 0)
    v_hi, v_lo = split(v_all.astype(F32) / V_SCALE)
    v_cat = jnp.concatenate([v_hi, v_lo, v_hi], axis=0)

    wide = cols(draws, f * 1024, 1024)
    ones = jnp.ones((rows, 16), BF16)
    left = jnp.concatenate([draws[:, a * 1024 :][:, :512] for a in range(4)], axis=1)

    def gram(a, b):
        return fence((dot(a, b, 0, 0) * G_SCALE).astype(F16))

    def gram_a(k0, k1):
        q0, q1 = (x + k0) % 4, (x + k1) % 4
        return gram(left, jnp.concatenate([cols(wide, q0 * 128, 128), cols(wide, 512 + q1 * 128, 128)], axis=1))

    def gram_b(k0, k1):
        q0, q1 = (z + k0) % 4, (z + k1) % 4
        first = cols(draws, q0 * 1024 + 512, 256)
        second = cols(draws, q1 * 1024 + 768, 256)
        return gram(jnp.concatenate([first, second, ones], axis=1), wide)

    b_plus, b_minus = gram_b(2, 1), gram_b(3, 2)
    a_plus, a_minus = gram_a(2, 1), gram_a(3, 2)
    b_both, a_both, b_own, a_own = gram_b(1, 3), gram_a(1, 3), gram_b(0, 0), gram_a(0, 0)
    b0, b1 = ring_reduce(b_plus, b_minus, b_both, b_own, "z", 0)
    a0, a1 = ring_reduce(a_plus, a_minus, a_both, a_own, "x", 1)
    a = jnp.concatenate([a0, a1], axis=1).reshape(4, 512, 256)
    b = jnp.concatenate([b0, b1], axis=0)
    b = jnp.stack(
        [jnp.concatenate([b[:, q * 128 :][:, :128], b[:, 512 + q * 128 :][:, :128]], axis=1) for q in range(4)]
    )
    tile_a = add(*lax.all_to_all(a, "z", 0, 0, tiled=True)).astype(F16)
    tile_b = add(*lax.all_to_all(b, "x", 0, 0, tiled=True)).astype(F16)
    tile_a = jnp.concatenate([tile_a, tile_b[512:]], axis=0)
    mine = jnp.where(yl == 0, tile_a, tile_b)
    theirs = flip(jnp.where(yl == 0, tile_b, tile_a), "yl")
    tile = add(mine, theirs).astype(F16)
    pieces = [pair(v, "c") for v in pair(tile, "yh")]
    tile = jnp.concatenate([v for p in pieces for v in p], axis=1).astype(F32)
    c_hi, c_lo = split(tile)
    c_cat = jnp.concatenate([c_hi, c_hi, c_lo], axis=1)

    t_part = dot(c_cat, v_cat, 1, 0)
    sent = pack(t_part[:512].reshape(4, 128, 1024), t_part[512:513][None])
    t, mean = unpack(lax.all_to_all(sent, "x", 0, 0, tiled=True))
    t, mean = t.sum(axis=0), mean.sum(axis=0) / (G_SCALE * total)
    own_sums = lax.dynamic_slice(tile, (512, (z * 2 + yl) * 128), (1, 128)).reshape(128, 1)
    t = (t - own_sums * mean) * (1.0 / (G_SCALE * (total - 1)))
    expected = mean[0] + drift_part

    t16 = pack(t)
    got = jnp.zeros((8 * 144, 512), F16)
    group = ("z", "yl", "yh", "c")
    for d in range(2):
        block = cols(t16, (yl ^ d) * 512, 512)
        for j in range(4):
            pairs = []
            for zz in range(4):
                for yy in range(2):
                    for ff in range(4):
                        pairs.append((zz * 8 + yy * 4 + ff, ff * 8 + (yy ^ d) * 4 + (zz + j) % 4))
            r = lax.ppermute(block, group, pairs)
            got = lax.dynamic_update_slice_in_dim(got, r, (((f - j) % 4) * 2 + (yl ^ d)) * 144, 0)
    t_hi, t_lo = split(unpack(got.reshape(8, 144, 512))[0].reshape(1024, 512))
    t_cat = jnp.concatenate([t_hi, t_hi, t_lo], axis=0)
    cov_part = dot(t_cat, v_cat, 0, 0)
    cov = unpack(lax.all_to_all(pack(cov_part.reshape(4, 128, 1024)), "x", 0, 0, tiled=True))[0]
    return cov.sum(axis=0), expected


def solution(mesh):
    torus = Mesh(mesh.devices.reshape(4, 2, 4, 2, 2), ("z", "yl", "x", "yh", "c"))
    in_specs = (P(SCEN, None), P(SCEN, FAC), P(FAC, None), P(FAC))
    out_specs = (P(SCEN, FAC), P(FAC))
    return jax.shard_map(
        on_device, mesh=torus, in_specs=in_specs, out_specs=out_specs, check_vma=False
    )
```

```python
import jax
import jax.numpy as jnp
from jax import lax
from jax.sharding import Mesh
from jax.sharding import PartitionSpec as P

SCEN = ("z", "yl", "x")
FAC = ("yh", "c")
F32, F16, BF16 = jnp.float32, jnp.float16, jnp.bfloat16
G_SCALE = 1.0 / 32.0
V_SCALE = 64.0
fence = lax.optimization_barrier


def dot(a, b, ca, cb):
    return lax.dot_general(a, b, (((ca,), (cb,)), ((), ())), preferred_element_type=F32)


def split(x):
    hi = lax.reduce_precision(x, 8, 7)
    return hi.astype(BF16), (x - hi).astype(BF16)


def shift(x, axis, k):
    n = lax.axis_size(axis)
    return lax.ppermute(x, axis, [(i, (i + k) % n) for i in range(n)])


def flip(x, axis):
    return lax.ppermute(x, axis, [(0, 1), (1, 0)])


def add(*xs):
    total = xs[0].astype(F32)
    for v in xs[1:]:
        total = total + v.astype(F32)
    return total


def cols(x, start, size):
    return lax.dynamic_slice_in_dim(x, start, size, 1)


def ring_reduce(plus, minus, both, own, axis, dim):
    cut = both.shape[dim] // 32 * 16
    from_prev = shift(plus, axis, 1)
    from_next = shift(minus, axis, -1)

    def halves(v):
        return lax.slice_in_dim(v, 0, cut, axis=dim), lax.slice_in_dim(v, cut, v.shape[dim], axis=dim)

    b0, b1 = halves(both)
    far0, near1 = halves(from_prev)
    near0, far1 = halves(from_next)
    sum0 = shift(add(b0, far0).astype(F16), axis, 1)
    sum1 = shift(add(b1, far1).astype(F16), axis, -1)
    o0, o1 = halves(own)
    return add(o0, near0, sum0).astype(F16), add(o1, near1, sum1).astype(F16)


def pair(x, axis):
    i = lax.axis_index(axis)
    other = flip(x, axis)
    return jnp.where(i == 0, x, other), jnp.where(i == 0, other, x)


def pack(x, extra=None):
    top = jnp.max(jnp.abs(x))
    if extra is not None:
        top = jnp.maximum(top, jnp.max(jnp.abs(extra)))
    e = jnp.clip(jnp.floor(jnp.log2(jnp.maximum(top, 1e-30))), -100.0, 120.0)
    scale = jnp.exp2(13.0 - e)
    rows = x.shape[-2]
    pads = [(0, 0, 0)] * (x.ndim - 2) + [(0, 8, 0), (0, 0, 0)]
    y = lax.pad(x * scale, jnp.float32(0), pads)
    at = lax.broadcasted_iota(jnp.int32, y.shape, y.ndim - 2)
    y = jnp.where(at == rows, e, y)
    if extra is not None:
        hi = lax.reduce_precision(extra * scale, 5, 10)
        y = jnp.where(at == rows + 1, hi, y)
        y = jnp.where(at == rows + 2, extra * scale - hi, y)
    return y.astype(F16)


def unpack(y):
    rows = y.shape[-2] - 8
    back = jnp.exp2(y[..., rows : rows + 1, :].astype(F32) - 13.0)
    return y[..., :rows, :].astype(F32) * back, (
        y[..., rows + 1 : rows + 2, :].astype(F32) + y[..., rows + 2 : rows + 3, :].astype(F32)
    ) * back


def on_device(draws, chol, exposures, drift):
    z, yl, x = (lax.axis_index(k) for k in SCEN)
    f = lax.axis_index(FAC)
    rows = draws.shape[0]
    total = rows * 32

    d_hi = lax.reduce_precision(drift, 8, 7)
    d_mid = lax.reduce_precision(drift - d_hi, 8, 7)
    d_lo = drift - d_hi - d_mid
    at = lax.broadcasted_iota(jnp.int32, (16, 1024), 0)
    tail = jnp.where(at == 0, d_hi, jnp.where(at == 1, d_mid, jnp.where(at == 2, d_lo, 0.0)))
    own = jnp.concatenate([chol, tail.astype(BF16)], axis=0)
    pieces = [pair(v, "c") for v in pair(own, "yh")]
    lower = jnp.concatenate([v for p in pieces for v in p], axis=1)
    v_own = dot(lower, exposures, 1, 1)
    drift_part = v_own[128] + v_own[129] + v_own[130]
    v16 = (v_own[:128] * V_SCALE).astype(F16)

    v_pair = jnp.concatenate(pair(v16, "yl"), axis=0)
    v_all = jnp.zeros((1024, 1024), F16)
    for k, v in ((0, v_pair), (3, shift(v_pair, "z", 1)), (1, shift(v_pair, "z", -1)), (2, shift(v_pair, "z", 2))):
        v_all = lax.dynamic_update_slice_in_dim(v_all, v, (z + k) % 4 * 256, 0)
    v_hi, v_lo = split(v_all.astype(F32) / V_SCALE)
    v_cat = jnp.concatenate([v_hi, v_lo, v_hi], axis=0)

    wide = cols(draws, f * 1024, 1024)
    ones = jnp.ones((rows, 16), BF16)
    left = jnp.concatenate([draws[:, a * 1024 :][:, :512] for a in range(4)], axis=1)

    def gram(a, b):
        return fence((dot(a, b, 0, 0) * G_SCALE).astype(F16))

    def gram_a(k0, k1):
        q0, q1 = (x + k0) % 4, (x + k1) % 4
        return gram(left, jnp.concatenate([cols(wide, q0 * 128, 128), cols(wide, 512 + q1 * 128, 128)], axis=1))

    def gram_b(k0, k1):
        q0, q1 = (z + k0) % 4, (z + k1) % 4
        first = cols(draws, q0 * 1024 + 512, 256)
        second = cols(draws, q1 * 1024 + 768, 256)
        return gram(jnp.concatenate([first, second, ones], axis=1), wide)

    b_plus, b_minus = gram_b(2, 1), gram_b(3, 2)
    a_plus, a_minus = gram_a(2, 1), gram_a(3, 2)
    b_both, a_both, b_own, a_own = gram_b(1, 3), gram_a(1, 3), gram_b(0, 0), gram_a(0, 0)
    b0, b1 = ring_reduce(b_plus, b_minus, b_both, b_own, "z", 0)
    a0, a1 = ring_reduce(a_plus, a_minus, a_both, a_own, "x", 1)
    a = jnp.concatenate([a0, a1], axis=1)
    b = jnp.concatenate([b0, b1], axis=0)
    a, b, v_cat = fence((a, b, v_cat))

    def slice_a(k):
        return lax.dynamic_slice_in_dim(a, (z + k) % 4 * 512, 512, 0)

    def slice_b(k):
        q = (x + k) % 4
        return jnp.concatenate([cols(b, q * 128, 128), cols(b, 512 + q * 128, 128)], axis=1)

    sent = fence(tuple(g(k) for g in (slice_a, slice_b) for k in (2, 1, 3)))
    tile_a = add(slice_a(0), *(shift(v, "z", k) for v, k in zip(sent[:3], (2, 1, 3))))
    tile_b = add(slice_b(0), *(shift(v, "x", k) for v, k in zip(sent[3:], (2, 1, 3))))
    tile_a = jnp.concatenate([tile_a, tile_b[512:]], axis=0).astype(F16)
    tile_b = tile_b.astype(F16)
    mine = jnp.where(yl == 0, tile_a, tile_b)
    theirs = jnp.where(yl == 0, tile_b, tile_a)
    mine, theirs = fence((mine, theirs))
    y = ("yl", "yh")
    near = lax.ppermute(theirs, y, [(0, 2), (2, 0), (1, 3), (3, 1)])
    cross = lax.ppermute(theirs, y, [(0, 3), (3, 0), (1, 2), (2, 1)])
    same = lax.ppermute(mine, y, [(0, 1), (1, 0), (2, 3), (3, 2)])
    here, there = add(mine, near).astype(F16), add(same, cross).astype(F16)
    yh, core = lax.axis_index("yh"), lax.axis_index("c")
    pieces = [pair(jnp.where(yh == 0, here, there), "c"), pair(jnp.where(yh == 0, there, here), "c")]
    tile = jnp.concatenate([v for p in pieces for v in p], axis=1).astype(F32)
    c_hi, c_lo = split(tile)
    c_cat = jnp.concatenate([c_hi, c_hi, c_lo], axis=1)

    t_part = dot(c_cat, v_cat, 1, 0)
    sent = pack(t_part[:512].reshape(4, 128, 1024), t_part[512:513][None])
    t, mean = unpack(lax.all_to_all(sent, "x", 0, 0, tiled=True))
    t, mean = t.sum(axis=0), mean.sum(axis=0) / (G_SCALE * total)
    own_sums = lax.dynamic_slice(tile, (512, (z * 2 + yl) * 128), (1, 128)).reshape(128, 1)
    t = (t - own_sums * mean) * (1.0 / (G_SCALE * (total - 1)))
    expected = mean[0] + drift_part

    t16 = pack(t)
    group = ("z", "yl", "yh", "c")
    blocks = fence(tuple(cols(t16, (yl ^ d) * 512, 512) for d in range(2)))
    half = []
    for d in range(2):
        for r in range(2):
            pairs = []
            for zz in range(4):
                for yy in range(2):
                    for ff in range(4):
                        to = (zz // 2 + r) % 2 * 2 + zz % 2
                        pairs.append((zz * 8 + yy * 4 + ff, ff * 8 + (yy ^ d) * 4 + to))
            half.append(lax.ppermute(blocks[d], group, pairs))
    half = jnp.concatenate(half, axis=0)
    other = flip(half, "c")
    got = jnp.zeros((8 * 136, 512), F16)
    for source, parity in ((half, core), (other, 1 - core)):
        for d in range(2):
            for r in range(2):
                row = (d * 2 + r) * 136
                z_from = (yh + r) % 2 * 2 + parity
                piece = source[row : row + 136]
                got = lax.dynamic_update_slice_in_dim(got, piece, (z_from * 2 + (yl ^ d)) * 136, 0)
    t_hi, t_lo = split(unpack(got.reshape(8, 136, 512))[0].reshape(1024, 512))
    t_cat = jnp.concatenate([t_hi, t_hi, t_lo], axis=0)
    cov_part = dot(t_cat, v_cat, 0, 0)
    cov = unpack(lax.all_to_all(pack(cov_part.reshape(4, 128, 1024)), "x", 0, 0, tiled=True))[0]
    return cov.sum(axis=0), expected


def solution(mesh):
    torus = Mesh(mesh.devices.reshape(4, 2, 4, 2, 2), ("z", "yl", "x", "yh", "c"))
    in_specs = (P(SCEN, None), P(SCEN, FAC), P(FAC, None), P(FAC))
    out_specs = (P(SCEN, FAC), P(FAC))
    return jax.shard_map(
        on_device, mesh=torus, in_specs=in_specs, out_specs=out_specs, check_vma=False
    )
```

```python
import jax
import jax.numpy as jnp
from jax import lax
from jax.sharding import Mesh
from jax.sharding import PartitionSpec as P

SCEN = ("z", "yl", "x")
FAC = ("yh", "c")
F32, F16, BF16 = jnp.float32, jnp.float16, jnp.bfloat16
G_SCALE = 1.0 / 32.0
V_SCALE = 64.0
fence = lax.optimization_barrier


def dot(a, b, ca, cb):
    return lax.dot_general(a, b, (((ca,), (cb,)), ((), ())), preferred_element_type=F32)


def split(x):
    hi = lax.reduce_precision(x, 8, 7)
    return hi.astype(BF16), (x - hi).astype(BF16)


def shift(x, axis, k):
    n = lax.axis_size(axis)
    return lax.ppermute(x, axis, [(i, (i + k) % n) for i in range(n)])


def flip(x, axis):
    return lax.ppermute(x, axis, [(0, 1), (1, 0)])


def add(*xs):
    total = xs[0].astype(F32)
    for v in xs[1:]:
        total = total + v.astype(F32)
    return total


def cols(x, start, size):
    return lax.dynamic_slice_in_dim(x, start, size, 1)


def halves(v, dim):
    cut = v.shape[dim] // 32 * 16
    return lax.slice_in_dim(v, 0, cut, axis=dim), lax.slice_in_dim(v, cut, v.shape[dim], axis=dim)


def ring_first(plus, minus, both, axis, dim):
    far0, near1 = halves(shift(plus, axis, 1), dim)
    near0, far1 = halves(shift(minus, axis, -1), dim)
    b0, b1 = halves(both, dim)
    return (near0, near1), fence((add(b0, far0).astype(F16), add(b1, far1).astype(F16)))


def ring_second(near, messages, own, axis, dim):
    sum0 = shift(messages[0], axis, 1)
    sum1 = shift(messages[1], axis, -1)
    o0, o1 = halves(own, dim)
    return add(o0, near[0], sum0).astype(F16), add(o1, near[1], sum1).astype(F16)


def pair(x, axis):
    i = lax.axis_index(axis)
    other = flip(x, axis)
    return jnp.where(i == 0, x, other), jnp.where(i == 0, other, x)


def pack(x, extra=None):
    top = jnp.max(jnp.abs(x))
    if extra is not None:
        top = jnp.maximum(top, jnp.max(jnp.abs(extra)))
    e = jnp.clip(jnp.floor(jnp.log2(jnp.maximum(top, 1e-30))), -100.0, 120.0)
    scale = jnp.exp2(13.0 - e)
    rows = x.shape[-2]
    pads = [(0, 0, 0)] * (x.ndim - 2) + [(0, 8, 0), (0, 0, 0)]
    y = lax.pad(x * scale, jnp.float32(0), pads)
    at = lax.broadcasted_iota(jnp.int32, y.shape, y.ndim - 2)
    y = jnp.where(at == rows, e, y)
    if extra is not None:
        hi = lax.reduce_precision(extra * scale, 5, 10)
        y = jnp.where(at == rows + 1, hi, y)
        y = jnp.where(at == rows + 2, extra * scale - hi, y)
    return y.astype(F16)


def unpack(y):
    rows = y.shape[-2] - 8
    back = jnp.exp2(y[..., rows : rows + 1, :].astype(F32) - 13.0)
    return y[..., :rows, :].astype(F32) * back, (
        y[..., rows + 1 : rows + 2, :].astype(F32) + y[..., rows + 2 : rows + 3, :].astype(F32)
    ) * back


def on_device(draws, chol, exposures, drift):
    z, yl, x = (lax.axis_index(k) for k in SCEN)
    f = lax.axis_index(FAC)
    rows = draws.shape[0]
    total = rows * 32

    d_hi = lax.reduce_precision(drift, 8, 7)
    d_mid = lax.reduce_precision(drift - d_hi, 8, 7)
    d_lo = drift - d_hi - d_mid
    at = lax.broadcasted_iota(jnp.int32, (16, 1024), 0)
    tail = jnp.where(at == 0, d_hi, jnp.where(at == 1, d_mid, jnp.where(at == 2, d_lo, 0.0)))
    own = jnp.concatenate([chol, tail.astype(BF16)], axis=0)
    yh, core = lax.axis_index("yh"), lax.axis_index("c")
    over = flip(own, "yh")
    both = jnp.where(yh == 0, jnp.stack([own, over]), jnp.stack([over, own]))
    lower = jnp.zeros((144, 4096), BF16)
    traded = flip(both, "c")
    for h in range(2):
        lower = lax.dynamic_update_slice_in_dim(lower, both[h], (h * 2 + core) * 1024, 1)
        lower = lax.dynamic_update_slice_in_dim(lower, traded[h], (h * 2 + 1 - core) * 1024, 1)

    wide = fence(cols(draws, f * 1024, 1024))
    ones = jnp.ones((rows, 16), BF16)
    left = fence(draws[:, :2048])

    def gram(a, b):
        return fence((dot(a, b, 0, 0) * G_SCALE).astype(F16))

    def cols_a(k0, k1):
        q0, q1 = (x + k0) % 4, (x + k1) % 4
        return [cols(wide, q0 * 128, 128), cols(wide, 512 + q1 * 128, 128)]

    def cols_b(k0, k1):
        q0, q1 = (z + k0) % 4, (z + k1) % 4
        return [cols(draws, 2048 + q0 * 512, 256), cols(draws, 2304 + q1 * 512, 256), ones]

    def gram_a(parts):
        return gram(left, fence(jnp.concatenate(parts, axis=1)))

    def gram_b(parts):
        return gram(fence(jnp.concatenate(parts, axis=1)), wide)

    b_plus, b_minus = gram_b(cols_b(2, 1)), gram_b(cols_b(3, 2))
    a_plus, a_minus = gram_a(cols_a(2, 1)), gram_a(cols_a(3, 2))
    b_both, b_own = gram_b(cols_b(1, 3)), gram_b(cols_b(0, 0))
    a_rest = gram_a(cols_a(1, 3) + cols_a(0, 0))
    b_near, b_next = ring_first(b_plus, b_minus, b_both, "z", 0)
    a_near, a_next = ring_first(a_plus, a_minus, a_rest[:, :256], "x", 1)
    a_next, lower = fence((a_next, lower))
    b0, b1 = ring_second(b_near, b_next, b_own, "z", 0)
    a0, a1 = ring_second(a_near, a_next, a_rest[:, 256:], "x", 1)

    v_own = dot(lower, exposures, 1, 1)
    drift_part = v_own[128] + v_own[129] + v_own[130]
    v16 = fence((v_own[:128] * V_SCALE).astype(F16))
    v_other = flip(v16, "yl")
    v_pair = jnp.concatenate([jnp.where(yl == 0, v16, v_other), jnp.where(yl == 0, v_other, v16)], axis=0)
    v_prev, v_next = shift(v_pair, "z", 1), shift(v_pair, "z", -1)
    v_far0, v_far1 = shift(v_prev[:128], "z", 1), shift(v_next[128:], "z", -1)
    v_all = jnp.zeros((1024, 1024), F16)
    for k, v in ((0, v_pair), (768, v_prev), (256, v_next), (512, v_far0), (640, v_far1)):
        v_all = lax.dynamic_update_slice_in_dim(v_all, v, (z * 256 + k) % 1024, 0)

    a = jnp.concatenate([a0, a1], axis=1)
    b = jnp.concatenate([b0, b1], axis=0)
    a, b = fence((a, b))

    def slice_a(k):
        return lax.dynamic_slice_in_dim(a, (z + k) % 4 * 512, 512, 0)

    def slice_b(k):
        q = (x + k) % 4
        return jnp.concatenate([cols(b, q * 128, 128), cols(b, 512 + q * 128, 128)], axis=1)

    sent = fence(tuple(g(k) for g in (slice_a, slice_b) for k in (2, 1, 3)))
    tile_a = add(slice_a(0), *(shift(v, "z", k) for v, k in zip(sent[:3], (2, 1, 3))))
    tile_b = add(slice_b(0), *(shift(v, "x", k) for v, k in zip(sent[3:], (2, 1, 3))))
    tile_a = jnp.concatenate([tile_a, tile_b[512:]], axis=0).astype(F16)
    tile_b = tile_b.astype(F16)
    mine = jnp.where(yl == 0, tile_a, tile_b)
    theirs = jnp.where(yl == 0, tile_b, tile_a)
    mine, theirs = fence((mine, theirs))
    y = ("yl", "yh")
    near = lax.ppermute(theirs, y, [(0, 2), (2, 0), (1, 3), (3, 1)])
    cross = lax.ppermute(theirs, y, [(0, 3), (3, 0), (1, 2), (2, 1)])
    same = lax.ppermute(mine, y, [(0, 1), (1, 0), (2, 3), (3, 2)])
    here, there = add(mine, near).astype(F16), add(same, cross).astype(F16)
    pieces = [pair(jnp.where(yh == 0, here, there), "c"), pair(jnp.where(yh == 0, there, here), "c")]
    tile = jnp.concatenate([v for p in pieces for v in p], axis=1).astype(F32)
    v_hi, v_lo = split(v_all.astype(F32) / V_SCALE)
    v_cat = jnp.concatenate([v_hi, v_lo, v_hi], axis=0)
    c_hi, c_lo = split(tile)
    c_cat = jnp.concatenate([c_hi, c_hi, c_lo], axis=1)

    t_part = dot(c_cat, v_cat, 1, 0)
    sent = pack(t_part[:512].reshape(4, 128, 1024), t_part[512:513][None])
    t, mean = unpack(lax.all_to_all(sent, "x", 0, 0, tiled=True))
    t, mean = t.sum(axis=0), mean.sum(axis=0) / (G_SCALE * total)
    own_sums = lax.dynamic_slice(tile, (512, (yl * 4 + z) * 128), (1, 128)).reshape(128, 1)
    t = (t - own_sums * mean) * (1.0 / (G_SCALE * (total - 1)))
    expected = mean[0] + drift_part

    t16 = pack(t)
    group = ("z", "yl", "yh", "c")
    blocks = fence(tuple(cols(t16, (yl ^ d) * 512, 512) for d in range(2)))
    half = []
    for d in range(2):
        for r in range(2):
            pairs = []
            for zz in range(4):
                for yy in range(2):
                    for ff in range(4):
                        to = (zz // 2 + r) % 2 * 2 + zz % 2
                        pairs.append((zz * 8 + yy * 4 + ff, ff * 8 + (yy ^ d) * 4 + to))
            half.append(lax.ppermute(blocks[d], group, pairs))
    half = jnp.concatenate(half, axis=0)
    other = flip(half, "c")
    got = jnp.zeros((8 * 136, 512), F16)
    for source, parity in ((half, core), (other, 1 - core)):
        for d in range(2):
            for r in range(2):
                row = (d * 2 + r) * 136
                z_from = (yh + r) % 2 * 2 + parity
                piece = source[row : row + 136]
                got = lax.dynamic_update_slice_in_dim(got, piece, ((yl ^ d) * 4 + z_from) * 136, 0)
    t_hi, t_lo = split(unpack(got.reshape(8, 136, 512))[0].reshape(1024, 512))
    t_cat = jnp.concatenate([t_hi, t_hi, t_lo], axis=0)
    cov_part = dot(t_cat, v_cat, 0, 0)
    cov = unpack(lax.all_to_all(pack(cov_part.reshape(4, 128, 1024)), "x", 0, 0, tiled=True))[0]
    return cov.sum(axis=0), expected


def solution(mesh):
    torus = Mesh(mesh.devices.reshape(4, 2, 4, 2, 2), ("z", "yl", "x", "yh", "c"))
    in_specs = (P(SCEN, None), P(SCEN, FAC), P(FAC, None), P(FAC))
    out_specs = (P(SCEN, FAC), P(FAC))
    return jax.shard_map(
        on_device, mesh=torus, in_specs=in_specs, out_specs=out_specs, check_vma=False
    )
```

```python
import jax
import jax.numpy as jnp
from jax import lax
from jax.sharding import Mesh
from jax.sharding import PartitionSpec as P

SCEN = ("z", "yl", "x")
FAC = ("yh", "c")
F32, F16, BF16 = jnp.float32, jnp.float16, jnp.bfloat16
G_SCALE = 1.0 / 32.0
V_SCALE = 64.0
fence = lax.optimization_barrier


def dot(a, b, ca, cb):
    return lax.dot_general(a, b, (((ca,), (cb,)), ((), ())), preferred_element_type=F32)


def split(x):
    hi = lax.reduce_precision(x, 8, 7)
    return hi.astype(BF16), (x - hi).astype(BF16)


def shift(x, axis, k):
    n = lax.axis_size(axis)
    return lax.ppermute(x, axis, [(i, (i + k) % n) for i in range(n)])


def flip(x, axis):
    return lax.ppermute(x, axis, [(0, 1), (1, 0)])


def add(*xs):
    total = xs[0].astype(F32)
    for v in xs[1:]:
        total = total + v.astype(F32)
    return total


def piece(x, start, size, axis):
    at = [0] * x.ndim
    at[axis] = start
    shape = list(x.shape)
    shape[axis] = size
    return lax.dynamic_slice(x, at, shape, allow_negative_indices=False)


def put(x, v, start, axis):
    at = [0] * x.ndim
    at[axis] = start
    return lax.dynamic_update_slice(x, v, at, allow_negative_indices=False)


def cols(x, start, size):
    return piece(x, start, size, 1)


def halves(v, dim):
    cut = v.shape[dim] // 32 * 16
    return lax.slice_in_dim(v, 0, cut, axis=dim), lax.slice_in_dim(v, cut, v.shape[dim], axis=dim)


def ring_first(plus, minus, both, axis, dim):
    from_prev = shift(plus, axis, 1)
    from_next = shift(minus, axis, -1)
    far0, near1 = halves(from_prev, dim)
    near0, far1 = halves(from_next, dim)
    b0, b1 = halves(both, dim)
    return (near0, near1), fence((add(b0, far0).astype(F16), add(b1, far1).astype(F16)))


def ring_second(near, messages, own, axis, dim):
    sum0 = shift(messages[0], axis, 1)
    sum1 = shift(messages[1], axis, -1)
    o0, o1 = halves(own, dim)
    return add(o0, near[0], sum0).astype(F16), add(o1, near[1], sum1).astype(F16)


def pack(x, extra=None):
    top = jnp.max(jnp.abs(x), axis=tuple(range(x.ndim - 1)), keepdims=True)
    if extra is not None:
        top = jnp.maximum(top, jnp.abs(extra))
    e = jnp.clip(jnp.floor(jnp.log2(jnp.maximum(top, 1e-30))), -100.0, 120.0)
    scale = jnp.exp2(13.0 - e)
    rows = x.shape[-2]
    pads = [(0, 0, 0)] * (x.ndim - 2) + [(0, 8, 0), (0, 0, 0)]
    y = lax.pad(x * scale, jnp.float32(0), pads)
    at = lax.broadcasted_iota(jnp.int32, y.shape, y.ndim - 2)
    y = jnp.where(at == rows, e, y)
    if extra is not None:
        hi = lax.reduce_precision(extra * scale, 5, 10)
        y = jnp.where(at == rows + 1, hi, y)
        y = jnp.where(at == rows + 2, extra * scale - hi, y)
    return y.astype(F16)


def unpack(y):
    rows = y.shape[-2] - 8
    back = jnp.exp2(y[..., rows : rows + 1, :].astype(F32) - 13.0)
    return y[..., :rows, :].astype(F32) * back, (
        y[..., rows + 1 : rows + 2, :].astype(F32) + y[..., rows + 2 : rows + 3, :].astype(F32)
    ) * back


def on_device(draws, chol, exposures, drift):
    z, yl, x = (lax.axis_index(k) for k in SCEN)
    f = lax.axis_index(FAC)
    rows = draws.shape[0]
    total = rows * 32

    d_hi = lax.reduce_precision(drift, 8, 7)
    d_mid = lax.reduce_precision(drift - d_hi, 8, 7)
    d_lo = drift - d_hi - d_mid
    at = lax.broadcasted_iota(jnp.int32, (16, 1024), 0)
    tail = jnp.where(at == 0, d_hi, jnp.where(at == 1, d_mid, jnp.where(at == 2, d_lo, 0.0)))
    own = jnp.concatenate([chol, tail.astype(BF16)], axis=0)
    yh, core = lax.axis_index("yh"), lax.axis_index("c")
    over = flip(own, "yh")
    both = jnp.where(yh == 0, jnp.stack([own, over]), jnp.stack([over, own]))
    lower = jnp.zeros((144, 4096), BF16)
    traded = flip(both, "c")
    for h in range(2):
        lower = put(lower, both[h], (h * 2 + core) * 1024, 1)
        lower = put(lower, traded[h], (h * 2 + 1 - core) * 1024, 1)

    wide = fence(cols(draws, f * 1024, 1024))
    ones = jnp.ones((rows, 16), BF16)

    def gram(a, b):
        return fence((dot(a, b, 0, 0) * G_SCALE).astype(F16))

    def cols_a(k0, k1):
        q0, q1 = (x + k0) & 3, (x + k1) & 3
        return fence(jnp.concatenate([cols(wide, q0 * 128, 128), cols(wide, q1 * 128 + 512, 128)], axis=1))

    def cols_b(k0, k1):
        q0, q1 = (z + k0) & 3, (z + k1) & 3
        parts = [cols(draws, 2048 + q0 * 512, 256), cols(draws, 2304 + q1 * 512, 256), ones]
        return fence(jnp.concatenate(parts, axis=1))

    b_plus, b_minus = gram(cols_b(2, 1), wide), gram(cols_b(3, 2), wide)
    b_plus, b_minus, after = fence((b_plus, b_minus, z))
    left = fence(jnp.where(after >= 0, draws[:, :2048], 0))
    a_plus, a_minus = gram(left, cols_a(2, 1)), gram(left, cols_a(3, 2))
    b_near, b_next = ring_first(b_plus, b_minus, gram(cols_b(1, 3), wide), "z", 0)
    b_next, rest = fence((b_next, cols_a(1, 3)))
    a_near, a_next = ring_first(a_plus, a_minus, gram(left, rest), "x", 1)
    a_next, rest_a, rest_b, lower = fence((a_next, cols_a(0, 0), cols_b(0, 0), lower))
    b0, b1 = ring_second(b_near, b_next, gram(rest_b, wide), "z", 0)
    a0, a1 = ring_second(a_near, a_next, gram(left, rest_a), "x", 1)

    v_own = dot(lower, exposures, 1, 1)
    drift_part = v_own[128] + v_own[129] + v_own[130]
    v16 = fence((v_own[:128] * V_SCALE).astype(F16))
    v_other = flip(v16, "yl")
    v_pair = jnp.concatenate([jnp.where(yl == 0, v16, v_other), jnp.where(yl == 0, v_other, v16)], axis=0)
    v_prev, v_next = shift(v_pair, "z", 1), shift(v_pair, "z", -1)
    v_far0, v_far1 = shift(v_prev[:128], "z", 1), shift(v_next[128:], "z", -1)
    v_all = jnp.zeros((1024, 1024), F16)
    for k, v in ((0, v_pair), (768, v_prev), (256, v_next), (512, v_far0), (640, v_far1)):
        v_all = put(v_all, v, (z * 256 + k) & 1023, 0)

    a = jnp.concatenate([a0, a1], axis=1)
    b = jnp.concatenate([b0, b1], axis=0)
    a, b = fence((a, b))

    def slice_a(k):
        return piece(a, ((z + k) & 3) * 512, 512, 0)

    def slice_b(k):
        q = (x + k) & 3
        return jnp.concatenate([cols(b, q * 128, 128), cols(b, q * 128 + 512, 128)], axis=1)

    sent = fence(tuple(g(k) for g in (slice_a, slice_b) for k in (2, 1, 3)))
    tile_a = add(slice_a(0), *(shift(v, "z", k) for v, k in zip(sent[:3], (2, 1, 3))))
    tile_b = add(slice_b(0), *(shift(v, "x", k) for v, k in zip(sent[3:], (2, 1, 3))))
    tile_a = jnp.concatenate([tile_a, tile_b[512:]], axis=0).astype(F16)
    tile_b = tile_b.astype(F16)
    mine = jnp.where(yl == 0, tile_a, tile_b)
    theirs = jnp.where(yl == 0, tile_b, tile_a)
    mine, theirs = fence((mine, theirs))
    y = ("yl", "yh")
    near = lax.ppermute(theirs, y, [(0, 2), (2, 0), (1, 3), (3, 1)])
    cross = lax.ppermute(theirs, y, [(0, 3), (3, 0), (1, 2), (2, 1)])
    same = lax.ppermute(mine, y, [(0, 1), (1, 0), (2, 3), (3, 2)])
    here, there = add(mine, near).astype(F16), add(same, cross).astype(F16)
    ours = jnp.concatenate([jnp.where(yh == 0, here, there), jnp.where(yh == 0, there, here)], axis=1)
    traded = flip(ours, "c")
    first, second = jnp.where(core == 0, ours, traded), jnp.where(core == 0, traded, ours)
    tile = jnp.concatenate([v[:, h * 256 :][:, :256] for h in range(2) for v in (first, second)], axis=1).astype(F32)
    v_hi, v_lo = split(v_all.astype(F32) / V_SCALE)
    v_cat = jnp.concatenate([v_hi, v_lo, v_hi], axis=0)
    c_hi, c_lo = split(tile)
    c_cat = jnp.concatenate([c_hi, c_hi, c_lo], axis=1)

    t_part = dot(c_cat, v_cat, 1, 0)
    sent = pack(t_part[:512].reshape(4, 128, 1024), t_part[512:513][None])
    t, mean = unpack(lax.all_to_all(sent, "x", 0, 0, tiled=True))
    t, mean = t.sum(axis=0), mean.sum(axis=0) / (G_SCALE * total)
    own_sums = cols(tile[512:513], (yl * 4 + z) * 128, 128).reshape(128, 1)
    t = (t - own_sums * mean) * (1.0 / (G_SCALE * (total - 1)))
    expected = mean[0] + drift_part

    t16 = pack(t)
    group = ("z", "yl", "yh", "c")
    blocks = fence(tuple(cols(t16, (yl ^ d) * 512, 512) for d in range(2)))
    half = []
    for d in range(2):
        for r in range(2):
            pairs = []
            for zz in range(4):
                for yy in range(2):
                    for ff in range(4):
                        to = (zz // 2 + r) % 2 * 2 + zz % 2
                        pairs.append((zz * 8 + yy * 4 + ff, ff * 8 + (yy ^ d) * 4 + to))
            half.append(lax.ppermute(blocks[d], group, pairs))
    half = jnp.concatenate(half, axis=0)
    other = flip(half, "c")
    got = jnp.zeros((8 * 136, 512), F16)
    for source, parity in ((half, core), (other, 1 - core)):
        for d in range(2):
            for r in range(2):
                row = (d * 2 + r) * 136
                z_from = (yh ^ r) * 2 + parity
                got = put(got, source[row : row + 136], ((yl ^ d) * 4 + z_from) * 136, 0)
    t_hi, t_lo = split(unpack(got.reshape(8, 136, 512))[0].reshape(1024, 512))
    t_cat = jnp.concatenate([t_hi, t_hi, t_lo], axis=0)
    cov_part = dot(t_cat, v_cat, 0, 0)
    cov = unpack(lax.all_to_all(pack(cov_part.reshape(4, 128, 1024)), "x", 0, 0, tiled=True))[0]
    return cov.sum(axis=0), expected


def solution(mesh):
    torus = Mesh(mesh.devices.reshape(4, 2, 4, 2, 2), ("z", "yl", "x", "yh", "c"))
    in_specs = (P(SCEN, None), P(SCEN, FAC), P(FAC, None), P(FAC))
    out_specs = (P(SCEN, FAC), P(FAC))
    return jax.shard_map(on_device, mesh=torus, in_specs=in_specs, out_specs=out_specs, check_vma=False)
```

```python
import jax
import jax.numpy as jnp
from jax import lax
from jax.sharding import Mesh
from jax.sharding import PartitionSpec as P

SCEN = ("z", "yl", "x")
FAC = ("yh", "c")
F32, F16, BF16 = jnp.float32, jnp.float16, jnp.bfloat16
G_SCALE = 1.0 / 32.0
V_SCALE = 64.0
fence = lax.optimization_barrier


def dot(a, b, ca, cb):
    return lax.dot_general(a, b, (((ca,), (cb,)), ((), ())), preferred_element_type=F32)


def split(x):
    hi = lax.reduce_precision(x, 8, 7)
    return hi.astype(BF16), (x - hi).astype(BF16)


def shift(x, axis, k):
    n = lax.axis_size(axis)
    return lax.ppermute(x, axis, [(i, (i + k) % n) for i in range(n)])


def flip(x, axis):
    return lax.ppermute(x, axis, [(0, 1), (1, 0)])


def add(*xs):
    total = xs[0].astype(F32)
    for v in xs[1:]:
        total = total + v.astype(F32)
    return total


def piece(x, start, size, axis):
    at = [0] * x.ndim
    at[axis] = start
    shape = list(x.shape)
    shape[axis] = size
    return lax.dynamic_slice(x, at, shape, allow_negative_indices=False)


def put(x, v, start, axis):
    at = [0] * x.ndim
    at[axis] = start
    return lax.dynamic_update_slice(x, v, at, allow_negative_indices=False)


def cols(x, start, size):
    return piece(x, start, size, 1)


def halves(v, dim):
    cut = v.shape[dim] // 32 * 16
    return lax.slice_in_dim(v, 0, cut, axis=dim), lax.slice_in_dim(v, cut, v.shape[dim], axis=dim)


def ring_first(plus, minus, both, axis, dim):
    from_prev = shift(plus, axis, 1)
    from_next = shift(minus, axis, -1)
    far0, near1 = halves(from_prev, dim)
    near0, far1 = halves(from_next, dim)
    b0, b1 = halves(both, dim)
    return (near0, near1), fence((add(b0, far0).astype(F16), add(b1, far1).astype(F16)))


def ring_second(near, messages, own, axis, dim):
    sum0 = shift(messages[0], axis, 1)
    sum1 = shift(messages[1], axis, -1)
    o0, o1 = halves(own, dim)
    return add(o0, near[0], sum0).astype(F16), add(o1, near[1], sum1).astype(F16)


def pack(x, extra=None):
    top = jnp.max(jnp.abs(x), axis=tuple(range(x.ndim - 1)), keepdims=True)
    if extra is not None:
        top = jnp.maximum(top, jnp.abs(extra))
    e = jnp.clip(jnp.floor(jnp.log2(jnp.maximum(top, 1e-30))), -100.0, 120.0)
    scale = jnp.exp2(13.0 - e)
    rows = x.shape[-2]
    pads = [(0, 0, 0)] * (x.ndim - 2) + [(0, 8, 0), (0, 0, 0)]
    y = lax.pad(x * scale, jnp.float32(0), pads)
    at = lax.broadcasted_iota(jnp.int32, y.shape, y.ndim - 2)
    y = jnp.where(at == rows, e, y)
    if extra is not None:
        hi = lax.reduce_precision(extra * scale, 5, 10)
        y = jnp.where(at == rows + 1, hi, y)
        y = jnp.where(at == rows + 2, extra * scale - hi, y)
    return y.astype(F16)


def unpack(y):
    rows = y.shape[-2] - 8
    back = jnp.exp2(y[..., rows : rows + 1, :].astype(F32) - 13.0)
    return y[..., :rows, :].astype(F32) * back, (
        y[..., rows + 1 : rows + 2, :].astype(F32) + y[..., rows + 2 : rows + 3, :].astype(F32)
    ) * back


def sum_over_x(packed, x):
    parts = [piece(packed, (x + k) & 3, 1, 0) for k in range(4)]
    sent = fence(tuple(parts[k] for k in (2, 1, 3)))
    got = [parts[0]] + [shift(v, "x", k) for v, k in zip(sent, (2, 1, 3))]
    rows, extra = zip(*(unpack(v[0]) for v in got))
    return sum(rows[1:], rows[0]), sum(extra[1:], extra[0])


def on_device(draws, chol, exposures, drift):
    z, yl, x = (lax.axis_index(k) for k in SCEN)
    f = lax.axis_index(FAC)
    rows = draws.shape[0]
    total = rows * 32

    d_hi = lax.reduce_precision(drift, 8, 7)
    d_mid = lax.reduce_precision(drift - d_hi, 8, 7)
    d_lo = drift - d_hi - d_mid
    at = lax.broadcasted_iota(jnp.int32, (16, 1024), 0)
    tail = jnp.where(at == 0, d_hi, jnp.where(at == 1, d_mid, jnp.where(at == 2, d_lo, 0.0)))
    own = jnp.concatenate([chol, tail.astype(BF16)], axis=0)
    yh, core = lax.axis_index("yh"), lax.axis_index("c")
    over = flip(own, "yh")
    both = jnp.where(yh == 0, jnp.stack([own, over]), jnp.stack([over, own]))
    lower = jnp.zeros((144, 4096), BF16)
    traded = flip(both, "c")
    for h in range(2):
        lower = put(lower, both[h], (h * 2 + core) * 1024, 1)
        lower = put(lower, traded[h], (h * 2 + 1 - core) * 1024, 1)

    wide = fence(cols(draws, f * 1024, 1024))
    ones = jnp.ones((rows, 16), BF16)

    def gram(a, b):
        return fence((dot(a, b, 0, 0) * G_SCALE).astype(F16))

    def cols_a(k0, k1):
        q0, q1 = (x + k0) & 3, (x + k1) & 3
        return fence(jnp.concatenate([cols(wide, q0 * 128, 128), cols(wide, q1 * 128 + 512, 128)], axis=1))

    def cols_b(k0, k1):
        q0, q1 = (z + k0) & 3, (z + k1) & 3
        parts = [cols(draws, 2048 + q0 * 512, 256), cols(draws, 2304 + q1 * 512, 256), ones]
        return fence(jnp.concatenate(parts, axis=1))

    b_plus, b_minus = gram(cols_b(2, 1), wide), gram(cols_b(3, 2), wide)
    b_plus, b_minus, after = fence((b_plus, b_minus, z))
    left = fence(jnp.where(after >= 0, draws[:, :2048], 0))
    a_plus, a_minus = gram(left, cols_a(2, 1)), gram(left, cols_a(3, 2))
    b_near, b_next = ring_first(b_plus, b_minus, gram(cols_b(1, 3), wide), "z", 0)
    b_next, rest = fence((b_next, cols_a(1, 3)))
    a_near, a_next = ring_first(a_plus, a_minus, gram(left, rest), "x", 1)
    a_next, rest_a, lower = fence((a_next, cols_a(0, 0), lower))
    b0, b1 = ring_second(b_near, b_next, gram(cols_b(0, 0), wide), "z", 0)
    a0, a1 = ring_second(a_near, a_next, gram(left, rest_a), "x", 1)

    v_own = dot(lower, exposures, 1, 1)
    drift_part = v_own[128] + v_own[129] + v_own[130]
    v16 = fence((v_own[:128] * V_SCALE).astype(F16))
    v_other = flip(v16, "yl")
    v_pair = jnp.concatenate([jnp.where(yl == 0, v16, v_other), jnp.where(yl == 0, v_other, v16)], axis=0)
    v_prev, v_next = shift(v_pair, "z", 1), shift(v_pair, "z", -1)
    v_far0, v_far1 = shift(v_prev[:128], "z", 1), shift(v_next[128:], "z", -1)
    v_all = jnp.zeros((1024, 1024), F16)
    for k, v in ((0, v_pair), (768, v_prev), (256, v_next), (512, v_far0), (640, v_far1)):
        v_all = put(v_all, v, (z * 256 + k) & 1023, 0)

    a = jnp.concatenate([a0, a1], axis=1)
    b = jnp.concatenate([b0, b1], axis=0)
    a, b = fence(a), fence(b)

    def slice_a(k):
        return piece(a, ((z + k) & 3) * 512, 512, 0)

    def slice_b(k):
        q = (x + k) & 3
        return jnp.concatenate([cols(b, q * 128, 128), cols(b, q * 128 + 512, 128)], axis=1)

    def hops(part, axis):
        sent = fence(tuple(part(k) for k in (2, 1, 3)))
        return [shift(v, axis, k) for v, k in zip(sent, (2, 1, 3))]

    from_b = hops(slice_b, "x")
    from_a = hops(slice_a, "z")
    tile_a = add(slice_a(0), *from_a)
    tile_b = add(slice_b(0), *from_b)
    tile_a = jnp.concatenate([tile_a, tile_b[512:]], axis=0).astype(F16)
    tile_b = tile_b.astype(F16)
    mine = jnp.where(yl == 0, tile_a, tile_b)
    theirs = jnp.where(yl == 0, tile_b, tile_a)
    mine, theirs = fence((mine, theirs))
    y = ("yl", "yh")
    near = lax.ppermute(theirs, y, [(0, 2), (2, 0), (1, 3), (3, 1)])
    cross = lax.ppermute(theirs, y, [(0, 3), (3, 0), (1, 2), (2, 1)])
    same = lax.ppermute(mine, y, [(0, 1), (1, 0), (2, 3), (3, 2)])
    here, there = add(mine, near).astype(F16), add(same, cross).astype(F16)
    ours = jnp.concatenate([jnp.where(yh == 0, here, there), jnp.where(yh == 0, there, here)], axis=1)
    traded = flip(ours, "c")
    first, second = jnp.where(core == 0, ours, traded), jnp.where(core == 0, traded, ours)
    tile = jnp.concatenate([v[:, h * 256 :][:, :256] for h in range(2) for v in (first, second)], axis=1).astype(F32)
    v_hi, v_lo = split(v_all.astype(F32) / V_SCALE)
    v_cat = jnp.concatenate([v_hi, v_lo, v_hi], axis=0)
    c_hi, c_lo = split(tile)
    c_cat = jnp.concatenate([c_hi, c_hi, c_lo], axis=1)

    t_part = dot(c_cat, v_cat, 1, 0)
    sent = pack(t_part[:512].reshape(4, 128, 1024), t_part[512:513][None])
    t, mean = sum_over_x(sent, x)
    mean = mean / (G_SCALE * total)
    own_sums = cols(tile[512:513], (yl * 4 + z) * 128, 128).reshape(128, 1)
    t = (t - own_sums * mean) * (1.0 / (G_SCALE * (total - 1)))
    expected = mean[0] + drift_part

    t16 = pack(t)
    group = ("z", "yl", "yh", "c")
    blocks = fence(tuple(cols(t16, (yl ^ d) * 512, 512) for d in range(2)))
    half = []
    for d in range(2):
        for r in range(2):
            pairs = []
            for zz in range(4):
                for yy in range(2):
                    for ff in range(4):
                        to = (zz // 2 + r) % 2 * 2 + zz % 2
                        pairs.append((zz * 8 + yy * 4 + ff, ff * 8 + (yy ^ d) * 4 + to))
            half.append(lax.ppermute(blocks[d], group, pairs))
    half = jnp.concatenate(half, axis=0)
    other = flip(half, "c")
    got = jnp.zeros((8 * 136, 512), F16)
    for source, parity in ((half, core), (other, 1 - core)):
        for d in range(2):
            for r in range(2):
                row = (d * 2 + r) * 136
                z_from = (yh ^ r) * 2 + parity
                got = put(got, source[row : row + 136], ((yl ^ d) * 4 + z_from) * 136, 0)
    t_hi, t_lo = split(unpack(got.reshape(8, 136, 512))[0].reshape(1024, 512))
    t_cat = jnp.concatenate([t_hi, t_hi, t_lo], axis=0)
    cov_part = dot(t_cat, v_cat, 0, 0)
    cov, _ = sum_over_x(pack(cov_part.reshape(4, 128, 1024)), x)
    return cov, expected


def solution(mesh):
    torus = Mesh(mesh.devices.reshape(4, 2, 4, 2, 2), ("z", "yl", "x", "yh", "c"))
    in_specs = (P(SCEN, None), P(SCEN, FAC), P(FAC, None), P(FAC))
    out_specs = (P(SCEN, FAC), P(FAC))
    return jax.shard_map(on_device, mesh=torus, in_specs=in_specs, out_specs=out_specs, check_vma=False)
```

```python
import jax
import jax.numpy as jnp
from jax import lax
from jax.sharding import Mesh
from jax.sharding import PartitionSpec as P

SCEN = ("z", "yl", "x")
FAC = ("yh", "c")
F32, F16, BF16 = jnp.float32, jnp.float16, jnp.bfloat16
G_SCALE = 1.0 / 32.0
V_SCALE = 64.0
fence = lax.optimization_barrier


def dot(a, b, ca, cb):
    return lax.dot_general(a, b, (((ca,), (cb,)), ((), ())), preferred_element_type=F32)


def split(x):
    hi = lax.reduce_precision(x, 8, 7)
    return hi.astype(BF16), (x - hi).astype(BF16)


def shift(x, axis, k):
    n = lax.axis_size(axis)
    return lax.ppermute(x, axis, [(i, (i + k) % n) for i in range(n)])


def flip(x, axis):
    return lax.ppermute(x, axis, [(0, 1), (1, 0)])


def add(*xs):
    total = xs[0].astype(F32)
    for v in xs[1:]:
        total = total + v.astype(F32)
    return total


def piece(x, start, size, axis):
    at = [0] * x.ndim
    at[axis] = start
    shape = list(x.shape)
    shape[axis] = size
    return lax.dynamic_slice(x, at, shape, allow_negative_indices=False)


def put(x, v, start, axis):
    at = [0] * x.ndim
    at[axis] = start
    return lax.dynamic_update_slice(x, v, at, allow_negative_indices=False)


def cols(x, start, size):
    return piece(x, start, size, 1)


def halves(v, dim):
    cut = v.shape[dim] // 32 * 16
    return lax.slice_in_dim(v, 0, cut, axis=dim), lax.slice_in_dim(v, cut, v.shape[dim], axis=dim)


def ring_first(plus, minus, both, axis, dim):
    from_prev = shift(plus, axis, 1)
    from_next = shift(minus, axis, -1)
    far0, near1 = halves(from_prev, dim)
    near0, far1 = halves(from_next, dim)
    b0, b1 = halves(both, dim)
    return (near0, near1), fence((add(b0, far0).astype(F16), add(b1, far1).astype(F16)))


def ring_second(near, messages, own, axis, dim):
    sum0 = shift(messages[0], axis, 1)
    sum1 = shift(messages[1], axis, -1)
    o0, o1 = halves(own, dim)
    return add(o0, near[0], sum0).astype(F16), add(o1, near[1], sum1).astype(F16)


def pack(x, extra=None):
    top = jnp.max(jnp.abs(x), axis=tuple(range(x.ndim - 1)), keepdims=True)
    if extra is not None:
        top = jnp.maximum(top, jnp.abs(extra))
    e = jnp.clip(jnp.floor(jnp.log2(jnp.maximum(top, 1e-30))), -100.0, 120.0)
    scale = jnp.exp2(13.0 - e)
    rows = x.shape[-2]
    pads = [(0, 0, 0)] * (x.ndim - 2) + [(0, 8, 0), (0, 0, 0)]
    y = lax.pad(x * scale, jnp.float32(0), pads)
    at = lax.broadcasted_iota(jnp.int32, y.shape, y.ndim - 2)
    y = jnp.where(at == rows, e, y)
    if extra is not None:
        hi = lax.reduce_precision(extra * scale, 5, 10)
        y = jnp.where(at == rows + 1, hi, y)
        y = jnp.where(at == rows + 2, extra * scale - hi, y)
    return y.astype(F16)


def unpack(y):
    rows = y.shape[-2] - 8
    back = jnp.exp2(y[..., rows : rows + 1, :].astype(F32) - 13.0)
    return y[..., :rows, :].astype(F32) * back, (
        y[..., rows + 1 : rows + 2, :].astype(F32) + y[..., rows + 2 : rows + 3, :].astype(F32)
    ) * back


def sum_over_x(packed, x):
    parts = [piece(packed, (x + k) & 3, 1, 0) for k in range(4)]
    sent = fence(tuple(parts[k] for k in (2, 1, 3)))
    got = [parts[0]] + [shift(v, "x", k) for v, k in zip(sent, (2, 1, 3))]
    rows, extra = zip(*(unpack(v[0]) for v in got))
    return sum(rows[1:], rows[0]), sum(extra[1:], extra[0])


def on_device(draws, chol, exposures, drift):
    z, yl, x = (lax.axis_index(k) for k in SCEN)
    f = lax.axis_index(FAC)
    rows = draws.shape[0]
    total = rows * 32

    d_hi = lax.reduce_precision(drift, 8, 7)
    d_mid = lax.reduce_precision(drift - d_hi, 8, 7)
    d_lo = drift - d_hi - d_mid
    at = lax.broadcasted_iota(jnp.int32, (16, 1024), 0)
    tail = jnp.where(at == 0, d_hi, jnp.where(at == 1, d_mid, jnp.where(at == 2, d_lo, 0.0)))
    own = jnp.concatenate([chol, tail.astype(BF16)], axis=0)
    yh, core = lax.axis_index("yh"), lax.axis_index("c")
    wide = fence(cols(draws, f * 1024, 1024))
    ones = jnp.ones((rows, 16), BF16)

    def gram(a, b):
        return fence((dot(a, b, 0, 0) * G_SCALE).astype(F16))

    def cols_a(k0, k1):
        q0, q1 = (x + k0) & 3, (x + k1) & 3
        return fence(jnp.concatenate([cols(wide, q0 * 128, 128), cols(wide, q1 * 128 + 512, 128)], axis=1))

    def cols_b(k0, k1, z):
        q0, q1 = (z + k0) & 3, (z + k1) & 3
        parts = [cols(draws, 2048 + q0 * 512, 256), cols(draws, 2304 + q1 * 512, 256), ones]
        return fence(jnp.concatenate(parts, axis=1))

    b_plus, b_minus = gram(cols_b(2, 1, z), wide), gram(cols_b(3, 2, z), wide)
    b_plus, b_minus, after = fence((b_plus, b_minus, z))
    left = fence(jnp.where(after >= 0, draws[:, :2048], 0))
    a_plus, a_minus = gram(left, cols_a(2, 1)), gram(left, cols_a(3, 2))
    a_plus, a_minus, own, late = fence((a_plus, a_minus, own, z))
    over = flip(own, "yh")
    both = jnp.where(yh == 0, jnp.stack([own, over]), jnp.stack([over, own]))
    lower = jnp.zeros((144, 4096), BF16)
    traded = flip(both, "c")
    for h in range(2):
        lower = put(lower, both[h], (h * 2 + core) * 1024, 1)
        lower = put(lower, traded[h], (h * 2 + 1 - core) * 1024, 1)

    b_near, b_next = ring_first(b_plus, b_minus, gram(cols_b(1, 3, late), wide), "z", 0)
    b_next, rest = fence((b_next, cols_a(1, 3)))
    a_near, a_next = ring_first(a_plus, a_minus, gram(left, rest), "x", 1)
    a_next, rest_a, lower = fence((a_next, cols_a(0, 0), lower))
    b0, b1 = ring_second(b_near, b_next, gram(cols_b(0, 0, late), wide), "z", 0)
    a0, a1 = ring_second(a_near, a_next, gram(left, rest_a), "x", 1)

    v_own = dot(lower, exposures, 1, 1)
    drift_part = v_own[128] + v_own[129] + v_own[130]
    v16 = fence((v_own[:128] * V_SCALE).astype(F16))
    v_other = flip(v16, "yl")
    v_pair = jnp.concatenate([jnp.where(yl == 0, v16, v_other), jnp.where(yl == 0, v_other, v16)], axis=0)
    v_prev, v_next = shift(v_pair, "z", 1), shift(v_pair, "z", -1)
    v_far0, v_far1 = shift(v_prev[:128], "z", 1), shift(v_next[128:], "z", -1)
    v_all = jnp.zeros((1024, 1024), F16)
    for k, v in ((0, v_pair), (768, v_prev), (256, v_next), (512, v_far0), (640, v_far1)):
        v_all = put(v_all, v, (z * 256 + k) & 1023, 0)

    a = jnp.concatenate([a0, a1], axis=1)
    b = jnp.concatenate([b0, b1], axis=0)
    a, b = fence(a), fence(b)

    def slice_a(k):
        return piece(a, ((z + k) & 3) * 512, 512, 0)

    def slice_b(k):
        q = (x + k) & 3
        return jnp.concatenate([cols(b, q * 128, 128), cols(b, q * 128 + 512, 128)], axis=1)

    def hops(part, axis):
        sent = fence(tuple(part(k) for k in (2, 1, 3)))
        return [shift(v, axis, k) for v, k in zip(sent, (2, 1, 3))]

    from_b = hops(slice_b, "x")
    from_a = hops(slice_a, "z")
    tile_a = add(slice_a(0), *from_a)
    tile_b = add(slice_b(0), *from_b)
    tile_a = jnp.concatenate([tile_a, tile_b[512:]], axis=0).astype(F16)
    tile_b = tile_b.astype(F16)
    mine = jnp.where(yl == 0, tile_a, tile_b)
    theirs = jnp.where(yl == 0, tile_b, tile_a)
    mine, theirs = fence((mine, theirs))
    y = ("yl", "yh")
    near = lax.ppermute(theirs, y, [(0, 2), (2, 0), (1, 3), (3, 1)])
    cross = lax.ppermute(theirs, y, [(0, 3), (3, 0), (1, 2), (2, 1)])
    same = lax.ppermute(mine, y, [(0, 1), (1, 0), (2, 3), (3, 2)])
    here, there = add(mine, near).astype(F16), add(same, cross).astype(F16)
    ours = jnp.concatenate([jnp.where(yh == 0, here, there), jnp.where(yh == 0, there, here)], axis=1)
    traded = flip(ours, "c")
    first, second = jnp.where(core == 0, ours, traded), jnp.where(core == 0, traded, ours)
    tile = jnp.concatenate([v[:, h * 256 :][:, :256] for h in range(2) for v in (first, second)], axis=1).astype(F32)
    v_hi, v_lo = split(v_all.astype(F32) / V_SCALE)
    v_cat = jnp.concatenate([v_hi, v_lo, v_hi], axis=0)
    c_hi, c_lo = split(tile)
    c_cat = jnp.concatenate([c_hi, c_hi, c_lo], axis=1)

    t_part = dot(c_cat, v_cat, 1, 0)
    sent = pack(t_part[:512].reshape(4, 128, 1024), t_part[512:513][None])
    t, mean = sum_over_x(sent, x)
    mean = mean / (G_SCALE * total)
    own_sums = cols(tile[512:513], (yl * 4 + z) * 128, 128).reshape(128, 1)
    t = (t - own_sums * mean) * (1.0 / (G_SCALE * (total - 1)))
    expected = mean[0] + drift_part

    t16 = pack(t)
    group = ("z", "yl", "yh", "c")
    blocks = fence(tuple(cols(t16, (yl ^ d) * 512, 512) for d in range(2)))
    half = {}
    for d in (1, 0):
        for r in (1, 0):
            pairs = []
            for zz in range(4):
                for yy in range(2):
                    for ff in range(4):
                        to = (zz // 2 + r) % 2 * 2 + zz % 2
                        pairs.append((zz * 8 + yy * 4 + ff, ff * 8 + (yy ^ d) * 4 + to))
            half[d * 2 + r] = lax.ppermute(blocks[d], group, pairs)
    half = jnp.concatenate([half[k] for k in range(4)], axis=0)
    other = flip(half, "c")
    got = jnp.zeros((8 * 136, 512), F16)
    for source, parity in ((half, core), (other, 1 - core)):
        for d in range(2):
            for r in range(2):
                row = (d * 2 + r) * 136
                z_from = (yh ^ r) * 2 + parity
                got = put(got, source[row : row + 136], ((yl ^ d) * 4 + z_from) * 136, 0)
    t_hi, t_lo = split(unpack(got.reshape(8, 136, 512))[0].reshape(1024, 512))
    t_cat = jnp.concatenate([t_hi, t_hi, t_lo], axis=0)
    cov_part = dot(t_cat, v_cat, 0, 0)
    cov, _ = sum_over_x(pack(cov_part.reshape(4, 128, 1024)), x)
    return cov, expected


def solution(mesh):
    torus = Mesh(mesh.devices.reshape(4, 2, 4, 2, 2), ("z", "yl", "x", "yh", "c"))
    in_specs = (P(SCEN, None), P(SCEN, FAC), P(FAC, None), P(FAC))
    out_specs = (P(SCEN, FAC), P(FAC))
    return jax.shard_map(on_device, mesh=torus, in_specs=in_specs, out_specs=out_specs, check_vma=False)
```

```python
import jax
import jax.numpy as jnp
from jax import lax
from jax.sharding import Mesh
from jax.sharding import PartitionSpec as P

SCEN = ("z", "yl", "x")
FAC = ("yh", "c")
F32, F16, BF16 = jnp.float32, jnp.float16, jnp.bfloat16
G_SCALE = 1.0 / 32.0
V_SCALE = 64.0
fence = lax.optimization_barrier


def dot(a, b, ca, cb):
    return lax.dot_general(a, b, (((ca,), (cb,)), ((), ())), preferred_element_type=F32)


def split(x):
    hi = lax.reduce_precision(x, 8, 7)
    return hi.astype(BF16), (x - hi).astype(BF16)


def shift(x, axis, k):
    n = lax.axis_size(axis)
    return lax.ppermute(x, axis, [(i, (i + k) % n) for i in range(n)])


def flip(x, axis):
    return lax.ppermute(x, axis, [(0, 1), (1, 0)])


def add(*xs):
    total = xs[0].astype(F32)
    for v in xs[1:]:
        total = total + v.astype(F32)
    return total


def piece(x, start, size, axis):
    at = [0] * x.ndim
    at[axis] = start
    shape = list(x.shape)
    shape[axis] = size
    return lax.dynamic_slice(x, at, shape, allow_negative_indices=False)


def put(x, v, start, axis):
    at = [0] * x.ndim
    at[axis] = start
    return lax.dynamic_update_slice(x, v, at, allow_negative_indices=False)


def cols(x, start, size):
    return piece(x, start, size, 1)


def halves(v, dim):
    cut = v.shape[dim] // 32 * 16
    return lax.slice_in_dim(v, 0, cut, axis=dim), lax.slice_in_dim(v, cut, v.shape[dim], axis=dim)


def ring_first(plus, minus, both, axis, dim):
    from_prev = shift(plus, axis, 1)
    from_next = shift(minus, axis, -1)
    far0, near1 = halves(from_prev, dim)
    near0, far1 = halves(from_next, dim)
    b0, b1 = halves(both, dim)
    return (near0, near1), fence((add(b0, far0).astype(F16), add(b1, far1).astype(F16)))


def ring_second(near, messages, own, axis, dim):
    sum0 = shift(messages[0], axis, 1)
    sum1 = shift(messages[1], axis, -1)
    o0, o1 = halves(own, dim)
    return add(o0, near[0], sum0).astype(F16), add(o1, near[1], sum1).astype(F16)


def pack(x, extra=None):
    top = jnp.max(jnp.abs(x), axis=tuple(range(x.ndim - 1)), keepdims=True)
    if extra is not None:
        top = jnp.maximum(top, jnp.abs(extra))
    e = jnp.clip(jnp.floor(jnp.log2(jnp.maximum(top, 1e-30))), -100.0, 120.0)
    scale = jnp.exp2(13.0 - e)
    rows = x.shape[-2]
    pads = [(0, 0, 0)] * (x.ndim - 2) + [(0, 8, 0), (0, 0, 0)]
    y = lax.pad(x * scale, jnp.float32(0), pads)
    at = lax.broadcasted_iota(jnp.int32, y.shape, y.ndim - 2)
    y = jnp.where(at == rows, e, y)
    if extra is not None:
        hi = lax.reduce_precision(extra * scale, 5, 10)
        y = jnp.where(at == rows + 1, hi, y)
        y = jnp.where(at == rows + 2, extra * scale - hi, y)
    return y.astype(F16)


def unpack(y):
    rows = y.shape[-2] - 8
    back = jnp.exp2(y[..., rows : rows + 1, :].astype(F32) - 13.0)
    return y[..., :rows, :].astype(F32) * back, (
        y[..., rows + 1 : rows + 2, :].astype(F32) + y[..., rows + 2 : rows + 3, :].astype(F32)
    ) * back


def sum_over_x(packed, x):
    parts = [piece(packed, (x + k) & 3, 1, 0) for k in range(4)]
    sent = fence(tuple(parts[k] for k in (2, 1, 3)))
    got = [parts[0]] + [shift(v, "x", k) for v, k in zip(sent, (2, 1, 3))]
    rows, extra = zip(*(unpack(v[0]) for v in got))
    return sum(rows[1:], rows[0]), sum(extra[1:], extra[0])


def on_device(draws, chol, exposures, drift):
    z, yl, x = (lax.axis_index(k) for k in SCEN)
    f = lax.axis_index(FAC)
    rows = draws.shape[0]
    total = rows * 32

    d_hi = lax.reduce_precision(drift, 8, 7)
    d_mid = lax.reduce_precision(drift - d_hi, 8, 7)
    d_lo = drift - d_hi - d_mid
    at = lax.broadcasted_iota(jnp.int32, (16, 1024), 0)
    tail = jnp.where(at == 0, d_hi, jnp.where(at == 1, d_mid, jnp.where(at == 2, d_lo, 0.0)))
    own = jnp.concatenate([chol, tail.astype(BF16)], axis=0)
    yh, core = lax.axis_index("yh"), lax.axis_index("c")
    wide = fence(cols(draws, f * 1024, 1024))
    ones = jnp.ones((rows, 16), BF16)

    def gram(a, b):
        return fence((dot(a, b, 0, 0) * G_SCALE).astype(F16))

    def cols_a(k0, k1):
        q0, q1 = (x + k0) & 3, (x + k1) & 3
        return fence(jnp.concatenate([cols(wide, q0 * 128, 128), cols(wide, q1 * 128 + 512, 128)], axis=1))

    def cols_b(k0, k1, z):
        q0, q1 = (z + k0) & 3, (z + k1) & 3
        parts = [cols(draws, 2048 + q0 * 512, 256), cols(draws, 2304 + q1 * 512, 256), ones]
        return fence(jnp.concatenate(parts, axis=1))

    b_plus, b_minus = gram(cols_b(2, 1, z), wide), gram(cols_b(3, 2, z), wide)
    b_plus, b_minus, after = fence((b_plus, b_minus, z))
    left = fence(jnp.where(after >= 0, draws[:, :2048], 0))
    a_plus, a_minus = gram(left, cols_a(2, 1)), gram(left, cols_a(3, 2))
    a_plus, a_minus, own, late = fence((a_plus, a_minus, own, z))
    over = flip(own, "yh")
    both = jnp.where(yh == 0, jnp.stack([own, over]), jnp.stack([over, own]))
    lower = jnp.zeros((144, 4096), BF16)
    traded = flip(both, "c")
    for h in range(2):
        lower = put(lower, both[h], (h * 2 + core) * 1024, 1)
        lower = put(lower, traded[h], (h * 2 + 1 - core) * 1024, 1)

    b_near, b_next = ring_first(b_plus, b_minus, gram(cols_b(1, 3, late), wide), "z", 0)
    b_next, rest = fence((b_next, cols_a(1, 3)))
    a_near, a_next = ring_first(a_plus, a_minus, gram(left, rest), "x", 1)
    a_next, rest_a, lower = fence((a_next, cols_a(0, 0), lower))
    b0, b1 = ring_second(b_near, b_next, gram(cols_b(0, 0, late), wide), "z", 0)
    a0, a1 = ring_second(a_near, a_next, gram(left, rest_a), "x", 1)

    v_own = dot(lower, exposures, 1, 1)
    drift_part = v_own[128] + v_own[129] + v_own[130]
    v16 = fence((v_own[:128] * V_SCALE).astype(F16))
    v_other = flip(v16, "yl")
    v_pair = jnp.concatenate([jnp.where(yl == 0, v16, v_other), jnp.where(yl == 0, v_other, v16)], axis=0)
    v_prev, v_next = shift(v_pair, "z", 1), shift(v_pair, "z", -1)
    v_far0, v_far1 = shift(v_prev[:128], "z", 1), shift(v_next[128:], "z", -1)
    v_all = jnp.zeros((1024, 1024), F16)
    for k, v in ((0, v_pair), (768, v_prev), (256, v_next), (512, v_far0), (640, v_far1)):
        v_all = put(v_all, v, (z * 256 + k) & 1023, 0)

    a = jnp.concatenate([a0, a1], axis=1)
    b = jnp.concatenate([b0, b1], axis=0)
    a, b = fence(a), fence(b)

    def slice_a(k):
        return piece(a, ((z + k) & 3) * 512, 512, 0)

    def slice_b(k):
        q = (x + k) & 3
        return jnp.concatenate([cols(b, q * 128, 128), cols(b, q * 128 + 512, 128)], axis=1)

    def hops(part, axis):
        sent = fence(tuple(part(k) for k in (2, 1, 3)))
        return [shift(v, axis, k) for v, k in zip(sent, (2, 1, 3))]

    from_b = hops(slice_b, "x")
    from_a = hops(slice_a, "z")
    tile_a = add(slice_a(0), *from_a)
    tile_b = add(slice_b(0), *from_b)
    tile_a = jnp.concatenate([tile_a, tile_b[512:]], axis=0).astype(F16)
    tile_b = tile_b.astype(F16)
    mine = jnp.where(yl == 0, tile_a, tile_b)
    theirs = jnp.where(yl == 0, tile_b, tile_a)
    mine, theirs = fence((mine, theirs))
    y = ("yl", "yh")
    near = lax.ppermute(theirs, y, [(0, 2), (2, 0), (1, 3), (3, 1)])
    cross = lax.ppermute(theirs, y, [(0, 3), (3, 0), (1, 2), (2, 1)])
    same = lax.ppermute(mine, y, [(0, 1), (1, 0), (2, 3), (3, 2)])
    here, there = add(mine, near).astype(F16), add(same, cross).astype(F16)
    ours = jnp.concatenate([jnp.where(yh == 0, here, there), jnp.where(yh == 0, there, here)], axis=1)
    traded = flip(ours, "c")
    first, second = jnp.where(core == 0, ours, traded), jnp.where(core == 0, traded, ours)
    tile = jnp.concatenate([v[:, h * 256 :][:, :256] for h in range(2) for v in (first, second)], axis=1).astype(F32)
    v_hi, v_lo = split(v_all.astype(F32) / V_SCALE)
    v_cat = jnp.concatenate([v_hi, v_lo, v_hi], axis=0)
    c_hi, c_lo = split(tile)
    c_cat = jnp.concatenate([c_hi, c_hi, c_lo], axis=1)

    t_part = dot(c_cat, v_cat, 1, 0)
    sent = pack(t_part[:512].reshape(4, 128, 1024), t_part[512:513][None])
    t, mean = sum_over_x(sent, x)
    mean = mean / (G_SCALE * total)
    own_sums = cols(tile[512:513], (yl * 4 + z) * 128, 128).reshape(128, 1)
    t = (t - own_sums * mean) * (1.0 / (G_SCALE * (total - 1)))
    expected = mean[0] + drift_part

    t16 = pack(t)
    group = ("z", "yl", "yh", "c")
    blocks = fence(tuple(cols(t16, (yl ^ d) * 512, 512) for d in range(2)))
    half = {}
    for d in (1, 0):
        for r in (1, 0):
            pairs = []
            for zz in range(4):
                for yy in range(2):
                    for ff in range(4):
                        to = (zz // 2 + r) % 2 * 2 + zz % 2
                        pairs.append((zz * 8 + yy * 4 + ff, ff * 8 + (yy ^ d) * 4 + to))
            half[d * 2 + r] = lax.ppermute(blocks[d], group, pairs)
    half = [half[k] for k in range(4)]
    other = [flip(v, "c") for v in half]
    got = jnp.zeros((8 * 136, 512), F16)
    for source, parity in ((half, core), (other, 1 - core)):
        for d in range(2):
            for r in range(2):
                z_from = (yh ^ r) * 2 + parity
                got = put(got, source[d * 2 + r], ((yl ^ d) * 4 + z_from) * 136, 0)
    t_hi, t_lo = split(unpack(got.reshape(8, 136, 512))[0].reshape(1024, 512))
    t_cat = jnp.concatenate([t_hi, t_hi, t_lo], axis=0)
    cov_part = dot(t_cat, v_cat, 0, 0)
    cov, _ = sum_over_x(pack(cov_part.reshape(4, 128, 1024)), x)
    return cov, expected


def solution(mesh):
    torus = Mesh(mesh.devices.reshape(4, 2, 4, 2, 2), ("z", "yl", "x", "yh", "c"))
    in_specs = (P(SCEN, None), P(SCEN, FAC), P(FAC, None), P(FAC))
    out_specs = (P(SCEN, FAC), P(FAC))
    return jax.shard_map(on_device, mesh=torus, in_specs=in_specs, out_specs=out_specs, check_vma=False)
```
